32 devices in a mesh: cuts: 4 (over x, core), stem: 8 (over z, y).
Axes of the slice: x: 2, y: 2, z: 4, core: 2. Of those that a mesh axis runs over, the one named last changes fastest.
Arguments:
- stems: bfloat16 [4, 8, 128, 2, 512], P('cuts', 'stem'), may hold values from -6 to 6
- branches: bfloat16 [2, 2, 2, 512, 512], replicated, may hold values from -0.1875 to 0.1875
- closing: bfloat16 [2, 2, 512, 256], replicated, may hold values from -0.09375 to 0.09375
- slice_values: int32 [4, 3], P('cuts'), may hold values from 0 to 1
- mode_perms: int32 [3, 9], replicated, may hold values from 0 to 8, each once within a row
- owner_map: int32 [4], replicated, may hold values from 0 to 3, each once
Outputs:
- open_amplitudes: float32 [8, 4, 2, 64, 128], P('stem', 'cuts')
The draws below stay inside these ranges and needn't reach their ends.
Inputs may be any that keep to these rules, and one draw needn't show every extreme that they name: `mode_perms`: each row is a permutation of the 9 modes. `owner_map`: a permutation of the owner indices.
All inputs are finite; a program needn't handle non-finite values.
Results may differ from the reference program's by a relative error of at most 0.017.
Values may be sent and summed in bfloat16 or wider, within the bound.
No kernel may reach another device: no remote copies, remote signals or barrier semaphores. Data moves between devices by JAX's collectives and lax.ppermute only.
A program may use at most 64 MiB of HBM per device.

```python
import jax
import jax.numpy as jnp
from jax import lax

MODES = 9
WIDTH = 512
HALF = 256
ROWS = 128
VARIANTS = 2
SLICES = 4
PIECE = 64
N_CUTS = 4
N_STEM = 8


def touch_ends(array, rng, least, top_value):
    spot = [jax.random.randint(jax.random.fold_in(rng, axis), (), 0, length) for axis, length in enumerate(array.shape)]
    longest = array.shape.index(max(array.shape))
    neighbour = spot[:longest] + [(spot[longest] + 1) % array.shape[longest]] + spot[longest + 1:]
    return array.at[tuple(spot)].set(least).at[tuple(neighbour)].set(top_value)


def steps_of(rng, extent, pieces, smallest, high):
    def one(dim, blocks):
        heights = jax.random.uniform(jax.random.fold_in(jax.random.fold_in(rng, 6), dim), (blocks,), jnp.float32, smallest / len(pieces), high / len(pieces))
        return jnp.repeat(jnp.exp(heights), extent[dim] // blocks).reshape((-1,) + (1,) * (len(extent) - dim - 1))

    loudness = one(*pieces[0])
    for cut in pieces[1:]:
        loudness = loudness * one(*cut)
    return loudness


def centred(key, shape, spread, bound, shards=(), held_as=jnp.bfloat16):
    values = spread * jax.random.normal(key, shape, jnp.float32)
    if shards:
        values = values * steps_of(key, shape, shards, -0.22, 0.18)
    return jnp.clip(values, -bound, bound).astype(held_as)


def setup_inputs(seed: int = 0) -> dict:
    key_list = jax.random.split(jax.random.key(seed), 7)
    stems = centred(key_list[0], (SLICES, N_STEM, ROWS, 2, WIDTH), 1.0, 6.0, ((0, 4), (1, 8)))
    branches = centred(key_list[1], (2, VARIANTS, 2, WIDTH, WIDTH), (2 * WIDTH) ** -0.5, 0.1875)
    closing = centred(key_list[2], (VARIANTS, 2, WIDTH, HALF), (2 * WIDTH * N_CUTS) ** -0.5, 0.09375)
    slice_values = touch_ends(jax.random.randint(key_list[3], (SLICES, 3), 0, VARIANTS), jax.random.fold_in(key_list[3], 1), 0, VARIANTS - 1).astype(jnp.int32)
    mode_perms = jax.vmap(lambda own: jax.random.permutation(own, MODES))(jax.random.split(key_list[4], 3)).reshape((3, MODES)).astype(jnp.int32)
    owner_map = jax.random.permutation(key_list[5], N_CUTS).astype(jnp.int32)
    return dict(stems=stems, branches=branches, closing=closing, slice_values=slice_values, mode_perms=mode_perms, owner_map=owner_map)


def spread_order(perm, width):
    column = jnp.arange(width, dtype=jnp.int32)
    result = jnp.zeros((width,), jnp.int32)
    for bit in range(perm.shape[0]):
        moved = jnp.bitwise_and(jnp.right_shift(column, bit), 1)
        result = result + jnp.left_shift(moved, perm[bit].astype(jnp.int32))
    return result


def complex_block(pair):
    real_part = pair[0]
    imag_part = pair[1]
    top = jnp.concatenate([real_part, imag_part], axis=1)
    bottom = jnp.concatenate([-imag_part, real_part], axis=1)
    return jnp.concatenate([top, bottom], axis=0)


def relabel(amps):
    groups = N_STEM
    high = ROWS // groups
    narrow = WIDTH // groups
    parts = amps.reshape(groups, high, groups, 2, groups, narrow)
    parts = jnp.transpose(parts, (4, 0, 1, 3, 2, 5))
    return parts.reshape(groups, ROWS, 2, WIDTH)


def absorb(state, perm, pair):
    order = spread_order(perm, WIDTH)
    permuted = jnp.take(state, order, axis=3)
    flat = permuted.reshape(N_STEM * ROWS, 2 * WIDTH)
    out = jnp.dot(flat, complex_block(pair), preferred_element_type=jnp.float32)
    return out.astype(jnp.bfloat16)


def reference(stems, branches, closing, slice_values, mode_perms, owner_map):
    def one_slice(total, inputs):
        stem, values = inputs
        first = absorb(stem, mode_perms[0], branches[0, values[0]]).reshape(N_STEM, ROWS, 2, WIDTH)
        second = absorb(relabel(first), mode_perms[1], branches[1, values[1]]).reshape(N_STEM, ROWS, 2, WIDTH)
        final = absorb(relabel(second), mode_perms[2], closing[values[2]])
        final = final.reshape(N_STEM, ROWS, 2, HALF).astype(jnp.float32)
        return total + final, None

    start = jnp.zeros((N_STEM, ROWS, 2, HALF), jnp.float32)
    total, unused = lax.scan(one_slice, start, (stems, slice_values))
    blocks = total.reshape(N_STEM, ROWS, 2, N_CUTS, PIECE)
    blocks = jnp.take(blocks, owner_map.astype(jnp.int32), axis=3)
    return jnp.transpose(blocks, (0, 3, 2, 4, 1))
```

```python
import functools

import jax
import jax.numpy as jnp
from jax import lax
from jax.experimental import pallas as pl
from jax.experimental.pallas import tpu as pltpu
from jax.sharding import PartitionSpec as P

BF16 = jnp.bfloat16
F32 = jnp.float32
LANES = 128


def spread(column, modes):
    result = jnp.zeros_like(column)
    for bit, mode in enumerate(modes):
        moved = jnp.bitwise_and(jnp.right_shift(column, bit), 1)
        result = result + jnp.left_shift(moved, mode)
    return result


def stem_kernel(
    groups, values, perms, owners, stems, branches, closing, send,
    first, second, last, orders, amps, flat, pieces, sems,
):
    rows, width = stems.shape[1], stems.shape[2]
    half = last.shape[2]
    narrow = width // groups
    high = rows // groups
    per_tile = LANES // narrow
    copies = (
        pltpu.make_async_copy(branches.at[0, values[0, 0]], first, sems.at[0]),
        pltpu.make_async_copy(branches.at[1, values[0, 1]], second, sems.at[1]),
        pltpu.make_async_copy(closing.at[values[0, 2]], last, sems.at[2]),
    )
    for copy in copies:
        copy.start()
    column = lax.broadcasted_iota(jnp.int32, (1, width), 1)
    entry = lax.broadcasted_iota(jnp.int32, (width, width), 0)
    for step in range(3):
        source = spread(column, [perms[step, bit] for bit in range(perms.shape[1])])
        orders[step] = jnp.where(entry == source, 1.0, 0.0).astype(BF16)

    def absorb(state, step, pair):
        permuted = jnp.dot(state, orders[step], preferred_element_type=F32).astype(BF16)
        by_real = jnp.dot(permuted, pair[0], preferred_element_type=F32)
        by_imag = jnp.dot(permuted, pair[1], preferred_element_type=F32)
        return by_real[:rows] - by_imag[rows:], by_imag[:rows] + by_real[rows:]

    lane = lax.broadcasted_iota(jnp.int32, (high, LANES), 1)

    def relabel(parts):
        for part in range(2):
            for tile in range(width // LANES):
                amps[part, tile] = parts[part][:, tile * LANES : (tile + 1) * LANES]
        for part in range(2):
            for tile in range(width // LANES):
                for start in range(0, groups, per_tile):
                    taken = [
                        amps[part, tile, pl.ds(start + k, high, stride=groups), :] for k in range(per_tile)
                    ]
                    for g in range(per_tile):
                        block = taken[g]
                        for k in range(per_tile):
                            if k != g:
                                moved = pltpu.roll(taken[k], ((k - g) % per_tile) * narrow, 1)
                                block = jnp.where(lane // narrow == k, moved, block)
                        row = part * rows + (tile * per_tile + g) * high
                        at = (start // per_tile) * LANES
                        flat[row : row + high, at : at + LANES] = block.astype(BF16)
        return flat[...]

    state = stems[...].reshape(2 * rows, width)
    copies[0].wait()
    state = relabel(absorb(state, 0, first))
    copies[1].wait()
    state = relabel(absorb(state, 1, second))
    copies[2].wait()
    real, imag = absorb(state, 2, last)
    piece = LANES // 2
    wide = lax.broadcasted_iota(jnp.int32, (rows, LANES), 1) < piece
    for tile in range(half // LANES):
        re = real[:, tile * LANES : (tile + 1) * LANES]
        im = imag[:, tile * LANES : (tile + 1) * LANES]
        pieces[2 * tile] = jnp.where(wide, re, pltpu.roll(im, piece, 1)).astype(BF16)
        pieces[2 * tile + 1] = jnp.where(wide, pltpu.roll(re, piece, 1), im).astype(BF16)
    for owner in range(send.shape[0]):
        send[owner] = pieces[owners[owner]]


def sum_kernel(groups, count, received, total):
    depth, columns = received.shape[0], total.shape[1]
    source = lax.broadcasted_iota(jnp.int32, (depth, columns), 0) % columns
    block = columns // groups
    s, t, x = source // block, (source % block) // count, source % count
    place = (t * groups + s) * count + x
    chosen = jnp.where(place == lax.broadcasted_iota(jnp.int32, (depth, columns), 1), 1.0, 0.0).astype(BF16)
    total[...] = lax.dot_general(
        received[...], chosen, (((0,), (0,)), ((), ())), preferred_element_type=F32
    )


def local_body(stems, branches, closing, slice_values, mode_perms, owner_map):
    groups = lax.axis_size("stem")
    cuts = lax.axis_size("cuts")
    rows, width, half = stems.shape[2], stems.shape[4], closing.shape[3]
    high = rows // groups
    state = jnp.transpose(stems[0, 0], (1, 0, 2))
    vmem, smem = pl.BlockSpec(memory_space=pltpu.VMEM), pl.BlockSpec(memory_space=pltpu.SMEM)
    hbm = pl.BlockSpec(memory_space=pl.ANY)
    send = pl.pallas_call(
        functools.partial(stem_kernel, groups),
        out_shape=jax.ShapeDtypeStruct((cuts, rows, LANES), BF16),
        in_specs=[smem, smem, smem, vmem, hbm, hbm],
        out_specs=vmem,
        scratch_shapes=[
            pltpu.VMEM((2, width, width), BF16),
            pltpu.VMEM((2, width, width), BF16),
            pltpu.VMEM((2, width, half), BF16),
            pltpu.VMEM((3, width, width), BF16),
            pltpu.VMEM((2, width // LANES, rows, LANES), F32),
            pltpu.VMEM((2 * rows, width), BF16),
            pltpu.VMEM((cuts, rows, LANES), BF16),
            pltpu.SemaphoreType.DMA((3,)),
        ],
        name="stem",
    )(slice_values, mode_perms, owner_map, state, branches, closing)
    send = send.reshape(cuts * groups, high, LANES)
    received = lax.all_to_all(send, ("cuts", "stem"), split_axis=0, concat_axis=0, tiled=True)
    total = pl.pallas_call(
        functools.partial(sum_kernel, groups, high // groups),
        out_shape=jax.ShapeDtypeStruct((LANES, rows), F32),
        in_specs=[vmem],
        out_specs=vmem,
        name="total",
    )(received.reshape(cuts * rows, LANES))
    return total.reshape(1, 1, 2, half // cuts, rows)


def absorb(state, perm, pair):
    width = pair.shape[1]
    column = jnp.arange(width, dtype=jnp.int32)
    source = spread(column, [perm[bit] for bit in range(perm.shape[0])])
    order = (column[:, None] == source[None, :]).astype(BF16)
    permuted = jnp.einsum("rpi,ij->prj", state, order, preferred_element_type=F32).astype(BF16)
    product = jnp.einsum("prj,qjk->pqrk", permuted, pair, preferred_element_type=F32)
    return jnp.stack([product[0, 0] - product[1, 1], product[0, 1] + product[1, 0]], axis=1).astype(BF16)


def exchange_body(stems, branches, closing, slice_values, mode_perms, owner_map):
    groups = lax.axis_size("stem")
    cuts = lax.axis_size("cuts")
    rows, width, half = stems.shape[2], stems.shape[4], closing.shape[3]
    high, narrow, piece = rows // groups, width // groups, half // cuts
    chosen = slice_values[0]
    begun = absorb(stems[0, 0], mode_perms[0], branches[0, chosen[0]])
    begun = begun.reshape(high, groups, 2, groups, narrow)
    state = jnp.transpose(begun, (3, 0, 2, 1, 4)).reshape(rows, 2, width)
    mixed = absorb(state, mode_perms[1], branches[1, chosen[1]])
    leaving = jnp.transpose(mixed.reshape(groups, high, 2, groups, narrow), (3, 0, 1, 2, 4))
    arrived = lax.all_to_all(leaving, "stem", split_axis=0, concat_axis=0, tiled=True)
    arrived = jnp.transpose(arrived, (1, 0, 2, 3, 4)).reshape(groups, high, groups, 2, narrow)
    state = jnp.transpose(arrived, (0, 1, 3, 2, 4)).reshape(rows, 2, width)
    final = absorb(state, mode_perms[2], closing[chosen[2]]).reshape(rows, 2, cuts, piece)
    send = jnp.transpose(jnp.take(final, owner_map, axis=2), (2, 1, 3, 0))
    received = lax.all_to_all(send, "cuts", split_axis=0, concat_axis=0, tiled=True)
    total = jnp.sum(received.reshape(cuts, 2, piece, rows).astype(F32), axis=0)
    return total.reshape(1, 1, 2, piece, rows)


def body(*args):
    groups = lax.axis_size("stem")
    rows, width, half = args[0].shape[2], args[0].shape[4], args[2].shape[3]
    high, narrow = rows // groups, width // groups
    local = high % groups == 0 and high % 16 == 0 and LANES % narrow == 0 and groups % (LANES // narrow) == 0
    local = local and 2 * half == LANES * lax.axis_size("cuts") and half % LANES == 0
    return local_body(*args) if local else exchange_body(*args)


def solution(mesh):
    in_specs = (P("cuts", "stem", None, None, None), P(), P(), P("cuts", None), P(), P())
    out_specs = P("stem", "cuts", None, None, None)
    return jax.shard_map(body, mesh=mesh, in_specs=in_specs, out_specs=out_specs, check_vma=False)
```

```python
import functools

import jax
import jax.numpy as jnp
from jax import lax
from jax.experimental import pallas as pl
from jax.experimental.pallas import tpu as pltpu
from jax.sharding import PartitionSpec as P

BF16 = jnp.bfloat16
F32 = jnp.float32
LANES = 128


def spread(column, modes):
    result = jnp.zeros_like(column)
    for bit, mode in enumerate(modes):
        moved = jnp.bitwise_and(jnp.right_shift(column, bit), 1)
        result = result + jnp.left_shift(moved, mode)
    return result


def stem_kernel(
    groups, values, perms, owners, stems, branches, closing, send,
    begun, first, second, last, orders, amps, flat, pieces, sems, loose,
):
    rows, width = amps.shape[2], first.shape[1]
    half = last.shape[2]
    narrow = width // groups
    high = rows // groups
    per_tile = LANES // narrow
    copies = (
        pltpu.make_async_copy(stems, begun, sems.at[3]),
        pltpu.make_async_copy(branches.at[0, values[0, 0]], first, sems.at[0]),
        pltpu.make_async_copy(branches.at[1, values[0, 1]], second, sems.at[1]),
        pltpu.make_async_copy(closing.at[values[0, 2]], last, sems.at[2]),
    )
    for copy in copies:
        copy.start()
    column = lax.broadcasted_iota(jnp.int32, (1, width), 1)
    entry = lax.broadcasted_iota(jnp.int32, (width, width), 0)
    for step in range(3):
        source = spread(column, [perms[step, bit] for bit in range(perms.shape[1])])
        orders[step] = jnp.where(entry == source, 1.0, 0.0).astype(BF16)

    def absorb(state, step, pair):
        permuted = jnp.dot(state, orders[step], preferred_element_type=F32).astype(BF16)
        by_real = jnp.dot(permuted, pair[0], preferred_element_type=F32)
        by_imag = jnp.dot(permuted, pair[1], preferred_element_type=F32)
        return by_real[:rows] - by_imag[rows:], by_imag[:rows] + by_real[rows:]

    lane = lax.broadcasted_iota(jnp.int32, (high, LANES), 1)

    def relabel(parts):
        for part in range(2):
            for tile in range(width // LANES):
                amps[part, tile] = parts[part][:, tile * LANES : (tile + 1) * LANES]
        for part in range(2):
            for tile in range(width // LANES):
                for start in range(0, groups, per_tile):
                    taken = [
                        amps[part, tile, pl.ds(start + k, high, stride=groups), :] for k in range(per_tile)
                    ]
                    for g in range(per_tile):
                        block = taken[g]
                        for k in range(per_tile):
                            if k != g:
                                moved = pltpu.roll(taken[k], ((k - g) % per_tile) * narrow, 1)
                                block = jnp.where(lane // narrow == k, moved, block)
                        row = part * rows + (tile * per_tile + g) * high
                        at = (start // per_tile) * LANES
                        flat[row : row + high, at : at + LANES] = block.astype(BF16)
        return flat[...]

    copies[0].wait()
    tiles = width // LANES
    loose[...] = begun[...].astype(F32)
    for part in range(2):
        for tile in range(tiles):
            taken = loose[pl.ds(2 * tile + part, rows, stride=2 * tiles), :]
            flat[part * rows : (part + 1) * rows, tile * LANES : (tile + 1) * LANES] = taken.astype(BF16)
    state = flat[...]
    copies[1].wait()
    state = relabel(absorb(state, 0, first))
    copies[2].wait()
    state = relabel(absorb(state, 1, second))
    copies[3].wait()
    real, imag = absorb(state, 2, last)
    piece = LANES // 2
    wide = lax.broadcasted_iota(jnp.int32, (rows, LANES), 1) < piece
    for tile in range(half // LANES):
        re = real[:, tile * LANES : (tile + 1) * LANES]
        im = imag[:, tile * LANES : (tile + 1) * LANES]
        pieces[2 * tile] = jnp.where(wide, re, pltpu.roll(im, piece, 1)).astype(BF16)
        pieces[2 * tile + 1] = jnp.where(wide, pltpu.roll(re, piece, 1), im).astype(BF16)
    for owner in range(send.shape[0]):
        send[owner] = pieces[owners[owner]]


def sum_kernel(groups, count, received, total):
    depth, columns = received.shape[0], total.shape[1]
    source = lax.broadcasted_iota(jnp.int32, (depth, columns), 0) % columns
    block = columns // groups
    s, t, x = source // block, (source % block) // count, source % count
    place = (t * groups + s) * count + x
    chosen = jnp.where(place == lax.broadcasted_iota(jnp.int32, (depth, columns), 1), 1.0, 0.0).astype(BF16)
    total[...] = lax.dot_general(
        received[...], chosen, (((0,), (0,)), ((), ())), preferred_element_type=F32
    )


def local_body(stems, branches, closing, slice_values, mode_perms, owner_map):
    groups = lax.axis_size("stem")
    cuts = lax.axis_size("cuts")
    rows, width, half = stems.shape[2], stems.shape[4], closing.shape[3]
    high = rows // groups
    state = jnp.transpose(stems.reshape(rows, 2, width // LANES, LANES), (0, 2, 1, 3)).reshape(-1, LANES)
    vmem, smem = pl.BlockSpec(memory_space=pltpu.VMEM), pl.BlockSpec(memory_space=pltpu.SMEM)
    hbm = pl.BlockSpec(memory_space=pl.ANY)
    send = pl.pallas_call(
        functools.partial(stem_kernel, groups),
        out_shape=pltpu.VMEM((cuts, rows, LANES), BF16),
        in_specs=[smem, smem, smem, hbm, hbm, hbm],
        out_specs=vmem,
        scratch_shapes=[
            pltpu.VMEM((2 * rows * width // LANES, LANES), BF16),
            pltpu.VMEM((2, width, width), BF16),
            pltpu.VMEM((2, width, width), BF16),
            pltpu.VMEM((2, width, half), BF16),
            pltpu.VMEM((3, width, width), BF16),
            pltpu.VMEM((2, width // LANES, rows, LANES), F32),
            pltpu.VMEM((2 * rows, width), BF16),
            pltpu.VMEM((cuts, rows, LANES), BF16),
            pltpu.SemaphoreType.DMA((4,)),
            pltpu.VMEM((2 * rows * width // LANES, LANES), F32),
        ],
        name="stem",
    )(slice_values, mode_perms, owner_map, state, branches, closing)
    send = send.reshape(cuts * groups, high, LANES)
    received = lax.all_to_all(send, ("cuts", "stem"), split_axis=0, concat_axis=0, tiled=True)
    total = pl.pallas_call(
        functools.partial(sum_kernel, groups, high // groups),
        out_shape=jax.ShapeDtypeStruct((LANES, rows), F32),
        in_specs=[vmem],
        out_specs=vmem,
        name="total",
    )(pltpu.with_memory_space_constraint(received.reshape(cuts * rows, LANES), pltpu.VMEM))
    return total.reshape(1, 1, 2, half // cuts, rows)


def absorb(state, perm, pair):
    width = pair.shape[1]
    column = jnp.arange(width, dtype=jnp.int32)
    source = spread(column, [perm[bit] for bit in range(perm.shape[0])])
    order = (column[:, None] == source[None, :]).astype(BF16)
    permuted = jnp.einsum("rpi,ij->prj", state, order, preferred_element_type=F32).astype(BF16)
    product = jnp.einsum("prj,qjk->pqrk", permuted, pair, preferred_element_type=F32)
    return jnp.stack([product[0, 0] - product[1, 1], product[0, 1] + product[1, 0]], axis=1).astype(BF16)


def exchange_body(stems, branches, closing, slice_values, mode_perms, owner_map):
    groups = lax.axis_size("stem")
    cuts = lax.axis_size("cuts")
    rows, width, half = stems.shape[2], stems.shape[4], closing.shape[3]
    high, narrow, piece = rows // groups, width // groups, half // cuts
    chosen = slice_values[0]
    begun = absorb(stems[0, 0], mode_perms[0], branches[0, chosen[0]])
    begun = begun.reshape(high, groups, 2, groups, narrow)
    state = jnp.transpose(begun, (3, 0, 2, 1, 4)).reshape(rows, 2, width)
    mixed = absorb(state, mode_perms[1], branches[1, chosen[1]])
    leaving = jnp.transpose(mixed.reshape(groups, high, 2, groups, narrow), (3, 0, 1, 2, 4))
    arrived = lax.all_to_all(leaving, "stem", split_axis=0, concat_axis=0, tiled=True)
    arrived = jnp.transpose(arrived, (1, 0, 2, 3, 4)).reshape(groups, high, groups, 2, narrow)
    state = jnp.transpose(arrived, (0, 1, 3, 2, 4)).reshape(rows, 2, width)
    final = absorb(state, mode_perms[2], closing[chosen[2]]).reshape(rows, 2, cuts, piece)
    send = jnp.transpose(jnp.take(final, owner_map, axis=2), (2, 1, 3, 0))
    received = lax.all_to_all(send, "cuts", split_axis=0, concat_axis=0, tiled=True)
    total = jnp.sum(received.reshape(cuts, 2, piece, rows).astype(F32), axis=0)
    return total.reshape(1, 1, 2, piece, rows)


def body(*args):
    groups = lax.axis_size("stem")
    rows, width, half = args[0].shape[2], args[0].shape[4], args[2].shape[3]
    high, narrow = rows // groups, width // groups
    local = high % groups == 0 and high % 16 == 0 and LANES % narrow == 0 and groups % (LANES // narrow) == 0
    local = local and 2 * half == LANES * lax.axis_size("cuts") and half % LANES == 0
    return local_body(*args) if local else exchange_body(*args)


def solution(mesh):
    in_specs = (P("cuts", "stem", None, None, None), P(), P(), P("cuts", None), P(), P())
    out_specs = P("stem", "cuts", None, None, None)
    return jax.shard_map(body, mesh=mesh, in_specs=in_specs, out_specs=out_specs, check_vma=False)
```

```python
import functools

import jax
import jax.numpy as jnp
from jax import lax
from jax.experimental import pallas as pl
from jax.experimental.pallas import tpu as pltpu
from jax.sharding import PartitionSpec as P

BF16 = jnp.bfloat16
F32 = jnp.float32
LANES = 128


def spread(column, modes):
    result = jnp.zeros_like(column)
    for bit, mode in enumerate(modes):
        moved = jnp.bitwise_and(jnp.right_shift(column, bit), 1)
        result = result + jnp.left_shift(moved, mode)
    return result


def stem_kernel(
    groups, values_in, perms_in, owners_in, stems, branches, closing, give, keep,
    values, perms, owners, begun, loose, first, second, last, orders, amps, flat, pieces, sems,
):
    rows, width = flat.shape[0] // 2, flat.shape[1]
    half = last.shape[2]
    narrow = width // groups
    high = rows // groups
    tiles = width // LANES
    per_tile = LANES // narrow

    def start(source, target, place):
        copy = pltpu.make_async_copy(source, target, sems.at[place])
        copy.start()
        return copy

    scalars = [
        start(values_in, values, 0),
        start(perms_in, perms, 1),
        start(owners_in, owners, 2),
    ]
    arriving = [start(stems.at[:, l], begun.at[l], 6 + l) for l in range(groups)]
    both = start(branches.at[0], first, 3)
    for copy in scalars:
        copy.wait()
    middle = start(branches.at[1, values[0, 1]], second, 4)
    final = start(closing.at[values[0, 2]], last, 5)

    column = lax.broadcasted_iota(jnp.int32, (1, width), 1)
    deep = 16
    entry = lax.broadcasted_iota(jnp.int32, (deep, width), 0)

    def make_order(step):
        source = spread(column, [perms[step, bit] for bit in range(perms.shape[1])])
        wanted = (jnp.broadcast_to(source, (deep, width)) - entry).astype(jnp.int16)
        for block in range(width // deep):
            orders[step, block * deep : (block + 1) * deep] = jnp.where(
                wanted == jnp.int16(block * deep), jnp.ones((), BF16), jnp.zeros((), BF16)
            )

    def permute(step):
        permuted = jnp.dot(flat[...], orders[step], preferred_element_type=F32).astype(BF16)
        re, im = permuted[:rows], permuted[rows:]
        return jnp.concatenate([jnp.concatenate([re, -im], axis=1), jnp.concatenate([im, re], axis=1)], axis=0)

    def products(state, pair):
        chunk = 2 * LANES
        matrix = pair[...].reshape(2 * width, pair.shape[2])
        for at in range(0, pair.shape[2], chunk):
            product = jnp.dot(state, matrix[:, at : at + chunk], preferred_element_type=F32)
            yield at // LANES, [product[:, k * LANES : (k + 1) * LANES] for k in range(chunk // LANES)]

    lane = lax.broadcasted_iota(jnp.int32, (high, LANES), 1)

    def relabel(part, tile, take):
        for start in range(0, groups, per_tile):
            taken = [take(start + k) for k in range(per_tile)]
            for g in range(per_tile):
                block = taken[g]
                for k in range(per_tile):
                    if k != g:
                        moved = pltpu.roll(taken[k], ((k - g) % per_tile) * narrow, 1)
                        block = jnp.where(lane // narrow == k, moved, block)
                row = part * rows + (tile * per_tile + g) * high
                at = (start // per_tile) * LANES
                flat[row : row + high, at : at + LANES] = block.astype(BF16)

    make_order(0)
    for copy in arriving:
        copy.wait()
    loose[...] = begun[...].astype(F32).reshape(loose.shape)
    for part in range(2):
        for tile in range(tiles):
            taken = loose[pl.ds(2 * tile + part, rows, stride=2 * tiles), :]
            flat[part * rows : (part + 1) * rows, tile * LANES : (tile + 1) * LANES] = taken.astype(BF16)
    state = permute(0)
    make_order(1)
    make_order(2)
    both.wait()
    for at, blocks in products(state, first.at[values[0, 0]]):
        for k, block in enumerate(blocks):
            for part in range(2):
                relabel(part, at + k, lambda l: block[part * rows + l * high : part * rows + (l + 1) * high])
    state = permute(1)
    middle.wait()
    for at, blocks in products(state, second):
        for k, block in enumerate(blocks):
            amps[at + k] = block
            for part in range(2):
                relabel(part, at + k, lambda l: amps[at + k, pl.ds(part * rows + l, high, stride=groups), :])
    state = permute(2)
    final.wait()
    piece = LANES // 2
    wide = lax.broadcasted_iota(jnp.int32, (rows, LANES), 1) < piece
    for at, blocks in products(state, last):
        for k, block in enumerate(blocks):
            re, im = block[:rows], block[rows:]
            pieces[2 * (at + k)] = jnp.where(wide, re, pltpu.roll(im, piece, 1)).astype(BF16)
            pieces[2 * (at + k) + 1] = jnp.where(wide, pltpu.roll(re, piece, 1), im).astype(BF16)
    side = lax.axis_index("cuts") % 2
    for pair in range(give.shape[0]):
        give[pair] = pieces[owners[2 * pair + 1 - side]]
        keep[pair] = pieces[owners[2 * pair + side]]


def pair_kernel(order, high, keep, came, send):
    for place, (pair, group) in enumerate(order):
        rows = slice(group * high, (group + 1) * high)
        total = keep[pair, rows].astype(F32) + came[pair, rows].astype(F32)
        send[place] = total.astype(BF16)


def sum_kernel(order, groups, received, total):
    high, columns = received.shape[1], total.shape[1]
    count = high // groups
    row = lax.broadcasted_iota(jnp.int32, (high, columns), 0)
    first = (row // count) * (groups * count) + row % count
    distance = (lax.broadcasted_iota(jnp.int32, (high, columns), 1) - first).astype(jnp.int16)
    chosen = [
        jnp.where(distance == jnp.int16(group * count), jnp.ones((), BF16), jnp.zeros((), BF16)) for _, group in order
    ]
    total[...] = lax.dot_general(
        received[...].reshape(-1, LANES),
        jnp.concatenate(chosen, axis=0),
        (((0,), (0,)), ((), ())),
        preferred_element_type=F32,
    )


def group_order(pairs, groups):
    order = [(pair, group) for pair in range(pairs) for group in range(groups)]
    return order[::-1]


def local_body(stems, branches, closing, slice_values, mode_perms, owner_map):
    groups = lax.axis_size("stem")
    cuts = lax.axis_size("cuts")
    rows, width, half = stems.shape[2], stems.shape[4], closing.shape[3]
    high = rows // groups
    state = jnp.transpose(stems.reshape(rows, 2, width // LANES, LANES), (0, 2, 1, 3)).reshape(high, groups, -1, LANES)
    vmem, hbm = pl.BlockSpec(memory_space=pltpu.VMEM), pl.BlockSpec(memory_space=pl.ANY)
    half_shape = pltpu.VMEM((cuts // 2, rows, LANES), BF16)
    give, keep = pl.pallas_call(
        functools.partial(stem_kernel, groups),
        out_shape=(half_shape, half_shape),
        in_specs=[hbm] * 6,
        out_specs=(vmem, vmem),
        scratch_shapes=[
            pltpu.SMEM(slice_values.shape, jnp.int32),
            pltpu.SMEM(mode_perms.shape, jnp.int32),
            pltpu.SMEM(owner_map.shape, jnp.int32),
            pltpu.VMEM((groups, high) + state.shape[2:], BF16),
            pltpu.VMEM((2 * rows * width // LANES, LANES), F32),
            pltpu.VMEM(branches.shape[1:], BF16),
            pltpu.VMEM(branches.shape[2:], BF16),
            pltpu.VMEM(closing.shape[1:], BF16),
            pltpu.VMEM((3, width, width), BF16),
            pltpu.VMEM((width // LANES, 2 * rows, LANES), F32),
            pltpu.VMEM((2 * rows, width), BF16),
            pltpu.VMEM((cuts, rows, LANES), BF16),
            pltpu.SemaphoreType.DMA((6 + groups,)),
        ],
        name="stem",
    )(slice_values, mode_perms, owner_map, state, branches, closing)
    came = lax.ppermute(give, "cuts", [(i, i ^ 1) for i in range(cuts)])
    order = group_order(cuts // 2, groups)
    in_vmem = lambda x: pltpu.with_memory_space_constraint(x, pltpu.VMEM)
    send = pl.pallas_call(
        functools.partial(pair_kernel, order, high),
        out_shape=pltpu.VMEM((len(order), high, LANES), BF16),
        in_specs=[vmem, vmem],
        out_specs=vmem,
        name="pair",
    )(in_vmem(keep), in_vmem(came))
    members = [[(2 * pair + side) * groups + group for pair, group in order] for side in range(2)]
    received = lax.all_to_all(
        send, ("cuts", "stem"), split_axis=0, concat_axis=0, axis_index_groups=members, tiled=True
    )
    total = pl.pallas_call(
        functools.partial(sum_kernel, order, groups),
        out_shape=jax.ShapeDtypeStruct((LANES, rows), F32),
        in_specs=[vmem],
        out_specs=vmem,
        name="total",
    )(in_vmem(received))
    return total.reshape(1, 1, 2, half // cuts, rows)


def absorb(state, perm, pair):
    width = pair.shape[1]
    column = jnp.arange(width, dtype=jnp.int32)
    source = spread(column, [perm[bit] for bit in range(perm.shape[0])])
    order = (column[:, None] == source[None, :]).astype(BF16)
    permuted = jnp.einsum("rpi,ij->prj", state, order, preferred_element_type=F32).astype(BF16)
    product = jnp.einsum("prj,qjk->pqrk", permuted, pair, preferred_element_type=F32)
    return jnp.stack([product[0, 0] - product[1, 1], product[0, 1] + product[1, 0]], axis=1).astype(BF16)


def exchange_body(stems, branches, closing, slice_values, mode_perms, owner_map):
    groups = lax.axis_size("stem")
    cuts = lax.axis_size("cuts")
    rows, width, half = stems.shape[2], stems.shape[4], closing.shape[3]
    high, narrow, piece = rows // groups, width // groups, half // cuts
    chosen = slice_values[0]
    begun = absorb(stems[0, 0], mode_perms[0], branches[0, chosen[0]])
    begun = begun.reshape(high, groups, 2, groups, narrow)
    state = jnp.transpose(begun, (3, 0, 2, 1, 4)).reshape(rows, 2, width)
    mixed = absorb(state, mode_perms[1], branches[1, chosen[1]])
    leaving = jnp.transpose(mixed.reshape(groups, high, 2, groups, narrow), (3, 0, 1, 2, 4))
    arrived = lax.all_to_all(leaving, "stem", split_axis=0, concat_axis=0, tiled=True)
    arrived = jnp.transpose(arrived, (1, 0, 2, 3, 4)).reshape(groups, high, groups, 2, narrow)
    state = jnp.transpose(arrived, (0, 1, 3, 2, 4)).reshape(rows, 2, width)
    final = absorb(state, mode_perms[2], closing[chosen[2]]).reshape(rows, 2, cuts, piece)
    send = jnp.transpose(jnp.take(final, owner_map, axis=2), (2, 1, 3, 0))
    received = lax.all_to_all(send, "cuts", split_axis=0, concat_axis=0, tiled=True)
    total = jnp.sum(received.reshape(cuts, 2, piece, rows).astype(F32), axis=0)
    return total.reshape(1, 1, 2, piece, rows)


def body(*args):
    groups = lax.axis_size("stem")
    rows, width, half = args[0].shape[2], args[0].shape[4], args[2].shape[3]
    high, narrow = rows // groups, width // groups
    local = high % groups == 0 and high % 16 == 0 and LANES % narrow == 0 and groups % (LANES // narrow) == 0
    local = local and 2 * half == LANES * lax.axis_size("cuts") and half % LANES == 0 and lax.axis_size("cuts") % 2 == 0
    return local_body(*args) if local else exchange_body(*args)


def solution(mesh):
    in_specs = (P("cuts", "stem", None, None, None), P(), P(), P("cuts", None), P(), P())
    out_specs = P("stem", "cuts", None, None, None)
    return jax.shard_map(body, mesh=mesh, in_specs=in_specs, out_specs=out_specs, check_vma=False)
```

```python
import functools

import jax
import jax.numpy as jnp
from jax import lax
from jax.experimental import pallas as pl
from jax.experimental.pallas import tpu as pltpu
from jax.sharding import PartitionSpec as P

BF16 = jnp.bfloat16
F32 = jnp.float32
LANES = 128


def spread(column, modes):
    result = jnp.zeros_like(column)
    for bit, mode in enumerate(modes):
        moved = jnp.bitwise_and(jnp.right_shift(column, bit), 1)
        result = result + jnp.left_shift(moved, mode)
    return result


def stem_kernel(
    groups, values_in, perms_in, owners_in, stems, branches, closing, give, keep,
    values, perms, owners, begun, loose, first, second, last, orders, begin, flat, amps, later, pieces, half_way, sems,
):
    rows, width = begin.shape[0] // 2, begin.shape[1]
    half = last.shape[2]
    narrow = width // groups
    high = rows // groups
    count = high // groups
    tiles = width // LANES
    per_tile = LANES // narrow
    chunk = 2 * LANES
    streams = width // chunk
    own = groups // streams
    part_rows = rows // streams

    def start(source, target, place):
        copy = pltpu.make_async_copy(source, target, sems.at[place])
        copy.start()
        return copy

    scalars = [
        start(values_in, values, 0),
        start(perms_in, perms, 1),
        start(owners_in, owners, 2),
    ]
    arriving = [start(stems.at[:, l], begun.at[l], 5 + l) for l in range(groups)]
    variants = branches.shape[1]
    pairs = [
        [start(branches.at[0, v, q], first.at[v, q], 5 + groups + q * variants + v) for v in range(variants)]
        for q in range(2)
    ]
    for copy in scalars:
        copy.wait()
    middle = start(branches.at[1, values[0, 1]], second, 3)
    final = start(closing.at[values[0, 2]], last, 4)

    column = lax.broadcasted_iota(jnp.int32, (1, width), 1)
    deep = 16
    entry = lax.broadcasted_iota(jnp.int32, (deep, width), 0)

    def make_order(step):
        source = spread(column, [perms[step, bit] for bit in range(perms.shape[1])])
        wanted = (jnp.broadcast_to(source, (deep, width)) - entry).astype(jnp.int16)
        for block in range(width // deep):
            orders[step, block * deep : (block + 1) * deep] = jnp.where(
                wanted == jnp.int16(block * deep), jnp.ones((), BF16), jnp.zeros((), BF16)
            )

    def permute(step, state):
        permuted = jnp.dot(state, orders[step], preferred_element_type=F32).astype(BF16)
        part = permuted.shape[0] // 2
        re, im = permuted[:part], permuted[part:]
        return permuted, jnp.concatenate([-im, re], axis=0)

    def product(factors, pair):
        state = jnp.concatenate(factors, axis=1)
        return jnp.dot(state, pair[...].reshape(-1, pair.shape[2]), preferred_element_type=F32)

    def relabel(taken, target, at, row):
        lane = lax.broadcasted_iota(jnp.int32, taken[0].shape, 1) // narrow
        blocks = []
        for g in range(per_tile):
            block = taken[g]
            for k in range(per_tile):
                if k != g:
                    moved = pltpu.roll(taken[k], ((k - g) % per_tile) * narrow, 1)
                    block = jnp.where(lane == k, moved, block)
            blocks.append(block)
        block = jnp.concatenate(blocks, axis=0).astype(BF16)
        target[row : row + block.shape[0], at * LANES : (at + 1) * LANES] = block

    def relabel_first(stream, y):
        for k in range(chunk // LANES):
            for part in range(2):
                for at in range(tiles):
                    taken = [
                        y[part * rows + l * high : part * rows + (l + 1) * high, k * LANES : (k + 1) * LANES]
                        for l in range(at * per_tile, (at + 1) * per_tile)
                    ]
                    relabel(taken, flat.at[stream], at, part * part_rows + k * per_tile * high)

    def relabel_second(stream, y):
        for tile in range(tiles):
            amps[stream, tile] = y[:, tile * LANES : (tile + 1) * LANES]
        for tile in range(tiles):
            for part in range(2):
                for at in range(tiles):
                    taken = [
                        amps[stream, tile, pl.ds(part * part_rows + l, own * count, stride=groups), :]
                        for l in range(at * per_tile, (at + 1) * per_tile)
                    ]
                    relabel(taken, later.at[stream], at, part * part_rows + tile * per_tile * own * count)

    make_order(0)
    for copy in arriving:
        copy.wait()
    loose[...] = begun[...].astype(F32).reshape(loose.shape)
    for part in range(2):
        for tile in range(tiles):
            taken = loose[pl.ds(2 * tile + part, rows, stride=2 * tiles), :]
            begin[part * rows : (part + 1) * rows, tile * LANES : (tile + 1) * LANES] = taken.astype(BF16)
    factors = permute(0, begin[...])
    make_order(1)
    make_order(2)
    chosen = first.at[values[0, 0]]
    for copy in pairs[0]:
        copy.wait()
    for i in range(streams):
        half_way[i] = jnp.dot(factors[0], chosen[0, :, i * chunk : (i + 1) * chunk], preferred_element_type=F32)
    for copy in pairs[1]:
        copy.wait()
    y = [
        half_way[i] + jnp.dot(factors[1], chosen[1, :, i * chunk : (i + 1) * chunk], preferred_element_type=F32)
        for i in range(streams)
    ]
    state = []
    for i in range(streams):
        relabel_first(i, y[i])
        state.append(permute(1, flat[i]))
    middle.wait()
    final.wait()
    y = [product(state[i], second) for i in range(streams)]
    state = []
    for i in range(streams):
        relabel_second(i, y[i])
        state.append(permute(2, later[i]))
    piece = LANES // 2
    wide = lax.broadcasted_iota(jnp.int32, (part_rows, LANES), 1) < piece
    depth = own * count
    for i in range(streams):
        y = product(state[i], last)
        for tile in range(half // LANES):
            re = y[:part_rows, tile * LANES : (tile + 1) * LANES]
            im = y[part_rows:, tile * LANES : (tile + 1) * LANES]
            for k, block in enumerate(
                (jnp.where(wide, re, pltpu.roll(im, piece, 1)), jnp.where(wide, pltpu.roll(re, piece, 1), im))
            ):
                pieces[2 * tile + k, :, i * depth : (i + 1) * depth] = block.reshape(groups, depth, LANES).astype(BF16)
    side = lax.axis_index("cuts") % 2
    for pair in range(give.shape[0]):
        give[pair] = pieces[owners[2 * pair + 1 - side]].reshape(rows, LANES)
        keep[pair] = pieces[owners[2 * pair + side]].reshape(rows, LANES)


def pair_kernel(order, high, keep, came, send):
    for place, (pair, group) in enumerate(order):
        rows = slice(group * high, (group + 1) * high)
        total = keep[pair, rows].astype(F32) + came[pair, rows].astype(F32)
        send[place] = total.astype(BF16)


def sum_kernel(order, groups, received, total):
    high, columns = received.shape[1], total.shape[1]
    count = high // groups
    row = lax.broadcasted_iota(jnp.int32, (high, columns), 0)
    first = (row // count) * (groups * count) + row % count
    distance = (lax.broadcasted_iota(jnp.int32, (high, columns), 1) - first).astype(jnp.int16)
    chosen = [
        jnp.where(distance == jnp.int16(group * count), jnp.ones((), BF16), jnp.zeros((), BF16)) for _, group in order
    ]
    total[...] = lax.dot_general(
        received[...].reshape(-1, LANES),
        jnp.concatenate(chosen, axis=0),
        (((0,), (0,)), ((), ())),
        preferred_element_type=F32,
    )


def group_order(pairs, groups):
    order = [(pair, group) for pair in range(pairs) for group in range(groups)]
    return order[::-1]


def local_body(stems, branches, closing, slice_values, mode_perms, owner_map):
    groups = lax.axis_size("stem")
    cuts = lax.axis_size("cuts")
    rows, width, half = stems.shape[2], stems.shape[4], closing.shape[3]
    high = rows // groups
    state = jnp.transpose(stems.reshape(rows, 2, width // LANES, LANES), (0, 2, 1, 3)).reshape(high, groups, -1, LANES)
    vmem, hbm = pl.BlockSpec(memory_space=pltpu.VMEM), pl.BlockSpec(memory_space=pl.ANY)
    streams = width // (2 * LANES)
    half_shape = pltpu.VMEM((cuts // 2, rows, LANES), BF16)
    give, keep = pl.pallas_call(
        functools.partial(stem_kernel, groups),
        out_shape=(half_shape, half_shape),
        in_specs=[hbm] * 6,
        out_specs=(vmem, vmem),
        scratch_shapes=[
            pltpu.SMEM(slice_values.shape, jnp.int32),
            pltpu.SMEM(mode_perms.shape, jnp.int32),
            pltpu.SMEM(owner_map.shape, jnp.int32),
            pltpu.VMEM((groups, high) + state.shape[2:], BF16),
            pltpu.VMEM((2 * rows * width // LANES, LANES), F32),
            pltpu.VMEM(branches.shape[1:], BF16),
            pltpu.VMEM(branches.shape[2:], BF16),
            pltpu.VMEM(closing.shape[1:], BF16),
            pltpu.VMEM((3, width, width), BF16),
            pltpu.VMEM((2 * rows, width), BF16),
            pltpu.VMEM((streams, 2 * rows // streams, width), BF16),
            pltpu.VMEM((streams, width // LANES, 2 * rows // streams, LANES), F32),
            pltpu.VMEM((streams, 2 * rows // streams, width), BF16),
            pltpu.VMEM((cuts, groups, high, LANES), BF16),
            pltpu.VMEM((streams, 2 * rows, width // streams), F32),
            pltpu.SemaphoreType.DMA((5 + groups + 2 * branches.shape[1],)),
        ],
        name="stem",
    )(slice_values, mode_perms, owner_map, state, branches, closing)
    came = lax.ppermute(give, "cuts", [(i, i ^ 1) for i in range(cuts)])
    order = group_order(cuts // 2, groups)
    in_vmem = lambda x: pltpu.with_memory_space_constraint(x, pltpu.VMEM)
    send = pl.pallas_call(
        functools.partial(pair_kernel, order, high),
        out_shape=pltpu.VMEM((len(order), high, LANES), BF16),
        in_specs=[vmem, vmem],
        out_specs=vmem,
        name="pair",
    )(in_vmem(keep), in_vmem(came))
    members = [[(2 * pair + side) * groups + group for pair, group in order] for side in range(2)]
    received = lax.all_to_all(
        send, ("cuts", "stem"), split_axis=0, concat_axis=0, axis_index_groups=members, tiled=True
    )
    total = pl.pallas_call(
        functools.partial(sum_kernel, order, groups),
        out_shape=jax.ShapeDtypeStruct((LANES, rows), F32),
        in_specs=[vmem],
        out_specs=vmem,
        name="total",
    )(in_vmem(received))
    return total.reshape(1, 1, 2, half // cuts, rows)


def absorb(state, perm, pair):
    width = pair.shape[1]
    column = jnp.arange(width, dtype=jnp.int32)
    source = spread(column, [perm[bit] for bit in range(perm.shape[0])])
    order = (column[:, None] == source[None, :]).astype(BF16)
    permuted = jnp.einsum("rpi,ij->prj", state, order, preferred_element_type=F32).astype(BF16)
    product = jnp.einsum("prj,qjk->pqrk", permuted, pair, preferred_element_type=F32)
    return jnp.stack([product[0, 0] - product[1, 1], product[0, 1] + product[1, 0]], axis=1).astype(BF16)


def exchange_body(stems, branches, closing, slice_values, mode_perms, owner_map):
    groups = lax.axis_size("stem")
    cuts = lax.axis_size("cuts")
    rows, width, half = stems.shape[2], stems.shape[4], closing.shape[3]
    high, narrow, piece = rows // groups, width // groups, half // cuts
    chosen = slice_values[0]
    begun = absorb(stems[0, 0], mode_perms[0], branches[0, chosen[0]])
    begun = begun.reshape(high, groups, 2, groups, narrow)
    state = jnp.transpose(begun, (3, 0, 2, 1, 4)).reshape(rows, 2, width)
    mixed = absorb(state, mode_perms[1], branches[1, chosen[1]])
    leaving = jnp.transpose(mixed.reshape(groups, high, 2, groups, narrow), (3, 0, 1, 2, 4))
    arrived = lax.all_to_all(leaving, "stem", split_axis=0, concat_axis=0, tiled=True)
    arrived = jnp.transpose(arrived, (1, 0, 2, 3, 4)).reshape(groups, high, groups, 2, narrow)
    state = jnp.transpose(arrived, (0, 1, 3, 2, 4)).reshape(rows, 2, width)
    final = absorb(state, mode_perms[2], closing[chosen[2]]).reshape(rows, 2, cuts, piece)
    send = jnp.transpose(jnp.take(final, owner_map, axis=2), (2, 1, 3, 0))
    received = lax.all_to_all(send, "cuts", split_axis=0, concat_axis=0, tiled=True)
    total = jnp.sum(received.reshape(cuts, 2, piece, rows).astype(F32), axis=0)
    return total.reshape(1, 1, 2, piece, rows)


def body(*args):
    groups = lax.axis_size("stem")
    rows, width, half = args[0].shape[2], args[0].shape[4], args[2].shape[3]
    high, narrow = rows // groups, width // groups
    local = high % groups == 0 and high % 16 == 0 and LANES % narrow == 0 and groups % (LANES // narrow) == 0
    local = local and 2 * half == LANES * lax.axis_size("cuts") and half % LANES == 0 and lax.axis_size("cuts") % 2 == 0
    return local_body(*args) if local else exchange_body(*args)


def solution(mesh):
    in_specs = (P("cuts", "stem", None, None, None), P(), P(), P("cuts", None), P(), P())
    out_specs = P("stem", "cuts", None, None, None)
    return jax.shard_map(body, mesh=mesh, in_specs=in_specs, out_specs=out_specs, check_vma=False)
```

```python
import functools

import jax
import jax.numpy as jnp
from jax import lax
from jax.experimental import pallas as pl
from jax.experimental.pallas import tpu as pltpu
from jax.sharding import PartitionSpec as P

BF16 = jnp.bfloat16
F32 = jnp.float32
LANES = 128


def spread(column, modes):
    result = jnp.zeros_like(column)
    for bit, mode in enumerate(modes):
        moved = jnp.bitwise_and(jnp.right_shift(column, bit), 1)
        result = result + jnp.left_shift(moved, mode)
    return result


def stem_kernel(
    groups, values_in, perms_in, owners_in, stems, branches, closing, give, keep,
    values, perms, owners, begun, loose, first, second, last, orders, begin, flat, amps, later, pieces, half_way, sems,
):
    rows, width = begin.shape[0] // 2, begin.shape[1]
    half = last.shape[2]
    narrow = width // groups
    high = rows // groups
    count = high // groups
    tiles = width // LANES
    per_tile = LANES // narrow
    chunk = 2 * LANES
    streams = width // chunk
    own = groups // streams
    part_rows = rows // streams

    def start(source, target, place):
        copy = pltpu.make_async_copy(source, target, sems.at[place])
        copy.start()
        return copy

    scalars = [
        start(values_in, values, 0),
        start(perms_in, perms, 1),
        start(owners_in, owners, 2),
    ]
    arriving = start(stems, begun, 5)
    pairs = [start(branches.at[0, :, q], first.at[:, q], 6 + q) for q in range(2)]
    for copy in scalars:
        copy.wait()
    middle = start(branches.at[1, values[0, 1]], second, 3)
    final = start(closing.at[values[0, 2]], last, 4)

    column = lax.broadcasted_iota(jnp.int32, (1, width), 1)
    packed = 16
    entry = lax.broadcasted_iota(jnp.int32, (packed, width), 0)

    def make_order(step):
        source = spread(column, [perms[step, bit] for bit in range(perms.shape[1])])
        wanted = (jnp.broadcast_to(source, (packed, width)) - entry).astype(jnp.int16)
        for block in range(width // packed):
            orders[step, block * packed : (block + 1) * packed] = jnp.where(
                wanted == jnp.int16(block * packed), jnp.ones((), BF16), jnp.zeros((), BF16)
            )

    def permute(step, state):
        permuted = jnp.dot(state, orders[step], preferred_element_type=F32).astype(BF16)
        part = permuted.shape[0] // 2
        re, im = permuted[:part], permuted[part:]
        return permuted, jnp.concatenate([-im, re], axis=0)

    def product(factors, pair):
        state = jnp.concatenate(factors, axis=1)
        return jnp.dot(state, pair[...].reshape(-1, pair.shape[2]), preferred_element_type=F32)

    def relabel(taken, target, at, row):
        lane = lax.broadcasted_iota(jnp.int32, taken[0].shape, 1) // narrow
        blocks = []
        for g in range(per_tile):
            block = taken[g]
            for k in range(per_tile):
                if k != g:
                    moved = pltpu.roll(taken[k], ((k - g) % per_tile) * narrow, 1)
                    block = jnp.where(lane == k, moved, block)
            blocks.append(block)
        block = jnp.concatenate(blocks, axis=0).astype(BF16)
        target[row : row + block.shape[0], at * LANES : (at + 1) * LANES] = block

    def relabel_first(stream, y):
        for k in range(chunk // LANES):
            for part in range(2):
                for at in range(tiles):
                    taken = [
                        y[part * rows + l * high : part * rows + (l + 1) * high, k * LANES : (k + 1) * LANES]
                        for l in range(at * per_tile, (at + 1) * per_tile)
                    ]
                    relabel(taken, flat.at[stream], at, part * part_rows + k * per_tile * high)

    def relabel_second(stream, y):
        for tile in range(tiles):
            amps[stream, tile] = y[:, tile * LANES : (tile + 1) * LANES]
        for tile in range(tiles):
            for part in range(2):
                for at in range(tiles):
                    taken = [
                        amps[stream, tile, pl.ds(part * part_rows + l, own * count, stride=groups), :]
                        for l in range(at * per_tile, (at + 1) * per_tile)
                    ]
                    relabel(taken, later.at[stream], at, part * part_rows + tile * per_tile * own * count)

    make_order(0)
    arriving.wait()
    deep = 2 * tiles * high
    for l in range(groups):
        loose[l * deep : (l + 1) * deep] = begun[:, l].astype(F32).reshape(deep, LANES)
    for part in range(2):
        for tile in range(tiles):
            taken = loose[pl.ds(2 * tile + part, rows, stride=2 * tiles), :]
            begin[part * rows : (part + 1) * rows, tile * LANES : (tile + 1) * LANES] = taken.astype(BF16)
    factors = permute(0, begin[...])
    make_order(1)
    make_order(2)
    chosen = first.at[values[0, 0]]
    pairs[0].wait()
    for i in range(streams):
        half_way[i] = jnp.dot(factors[0], chosen[0, :, i * chunk : (i + 1) * chunk], preferred_element_type=F32)
    pairs[1].wait()
    y = [
        half_way[i] + jnp.dot(factors[1], chosen[1, :, i * chunk : (i + 1) * chunk], preferred_element_type=F32)
        for i in range(streams)
    ]
    state = []
    for i in range(streams):
        relabel_first(i, y[i])
        state.append(permute(1, flat[i]))
    middle.wait()
    final.wait()
    y = [product(state[i], second) for i in range(streams)]
    state = []
    for i in range(streams):
        relabel_second(i, y[i])
        state.append(permute(2, later[i]))
    piece = LANES // 2
    wide = lax.broadcasted_iota(jnp.int32, (part_rows, LANES), 1) < piece
    depth = own * count
    for i in range(streams):
        y = product(state[i], last)
        for tile in range(half // LANES):
            re = y[:part_rows, tile * LANES : (tile + 1) * LANES]
            im = y[part_rows:, tile * LANES : (tile + 1) * LANES]
            for k, block in enumerate(
                (jnp.where(wide, re, pltpu.roll(im, piece, 1)), jnp.where(wide, pltpu.roll(re, piece, 1), im))
            ):
                pieces[2 * tile + k, :, i * depth : (i + 1) * depth] = block.reshape(groups, depth, LANES).astype(BF16)
    side = lax.axis_index("cuts") % 2
    for pair in range(give.shape[0]):
        give[pair] = pieces[owners[2 * pair + 1 - side]].reshape(rows, LANES)
        keep[pair] = pieces[owners[2 * pair + side]].reshape(rows, LANES)


def pair_kernel(order, high, keep, came, send):
    for place, (pair, group) in enumerate(order):
        rows = slice(group * high, (group + 1) * high)
        total = keep[pair, rows].astype(F32) + came[pair, rows].astype(F32)
        send[place] = total.astype(BF16)


def sum_kernel(order, groups, received, total):
    high, columns = received.shape[1], total.shape[1]
    count = high // groups
    row = lax.broadcasted_iota(jnp.int32, (high, columns), 0)
    first = (row // count) * (groups * count) + row % count
    distance = (lax.broadcasted_iota(jnp.int32, (high, columns), 1) - first).astype(jnp.int16)
    chosen = [
        jnp.where(distance == jnp.int16(group * count), jnp.ones((), BF16), jnp.zeros((), BF16)) for _, group in order
    ]
    total[...] = lax.dot_general(
        received[...].reshape(-1, LANES),
        jnp.concatenate(chosen, axis=0),
        (((0,), (0,)), ((), ())),
        preferred_element_type=F32,
    )


def group_order(pairs, groups):
    order = [(pair, group) for pair in range(pairs) for group in range(groups)]
    return order[::-1]


def local_body(stems, branches, closing, slice_values, mode_perms, owner_map):
    groups = lax.axis_size("stem")
    cuts = lax.axis_size("cuts")
    rows, width, half = stems.shape[2], stems.shape[4], closing.shape[3]
    high = rows // groups
    state = jnp.transpose(stems.reshape(rows, 2, width // LANES, LANES), (0, 2, 1, 3)).reshape(high, groups, -1, LANES)
    vmem, hbm = pl.BlockSpec(memory_space=pltpu.VMEM), pl.BlockSpec(memory_space=pl.ANY)
    streams = width // (2 * LANES)
    half_shape = pltpu.VMEM((cuts // 2, rows, LANES), BF16)
    give, keep = pl.pallas_call(
        functools.partial(stem_kernel, groups),
        out_shape=(half_shape, half_shape),
        in_specs=[hbm] * 6,
        out_specs=(vmem, vmem),
        scratch_shapes=[
            pltpu.SMEM(slice_values.shape, jnp.int32),
            pltpu.SMEM(mode_perms.shape, jnp.int32),
            pltpu.SMEM(owner_map.shape, jnp.int32),
            pltpu.VMEM(state.shape, BF16),
            pltpu.VMEM((2 * rows * width // LANES, LANES), F32),
            pltpu.VMEM(branches.shape[1:], BF16),
            pltpu.VMEM(branches.shape[2:], BF16),
            pltpu.VMEM(closing.shape[1:], BF16),
            pltpu.VMEM((3, width, width), BF16),
            pltpu.VMEM((2 * rows, width), BF16),
            pltpu.VMEM((streams, 2 * rows // streams, width), BF16),
            pltpu.VMEM((streams, width // LANES, 2 * rows // streams, LANES), F32),
            pltpu.VMEM((streams, 2 * rows // streams, width), BF16),
            pltpu.VMEM((cuts, groups, high, LANES), BF16),
            pltpu.VMEM((streams, 2 * rows, width // streams), F32),
            pltpu.SemaphoreType.DMA((8,)),
        ],
        name="stem",
    )(slice_values, mode_perms, owner_map, state, branches, closing)
    came = lax.ppermute(give, "cuts", [(i, i ^ 1) for i in range(cuts)])
    order = group_order(cuts // 2, groups)
    in_vmem = lambda x: pltpu.with_memory_space_constraint(x, pltpu.VMEM)
    send = pl.pallas_call(
        functools.partial(pair_kernel, order, high),
        out_shape=pltpu.VMEM((len(order), high, LANES), BF16),
        in_specs=[vmem, vmem],
        out_specs=vmem,
        name="pair",
    )(in_vmem(keep), in_vmem(came))
    members = [[(2 * pair + side) * groups + group for pair, group in order] for side in range(2)]
    received = lax.all_to_all(
        send, ("cuts", "stem"), split_axis=0, concat_axis=0, axis_index_groups=members, tiled=True
    )
    total = pl.pallas_call(
        functools.partial(sum_kernel, order, groups),
        out_shape=jax.ShapeDtypeStruct((LANES, rows), F32),
        in_specs=[vmem],
        out_specs=vmem,
        name="total",
    )(in_vmem(received))
    return total.reshape(1, 1, 2, half // cuts, rows)


def absorb(state, perm, pair):
    width = pair.shape[1]
    column = jnp.arange(width, dtype=jnp.int32)
    source = spread(column, [perm[bit] for bit in range(perm.shape[0])])
    order = (column[:, None] == source[None, :]).astype(BF16)
    permuted = jnp.einsum("rpi,ij->prj", state, order, preferred_element_type=F32).astype(BF16)
    product = jnp.einsum("prj,qjk->pqrk", permuted, pair, preferred_element_type=F32)
    return jnp.stack([product[0, 0] - product[1, 1], product[0, 1] + product[1, 0]], axis=1).astype(BF16)


def exchange_body(stems, branches, closing, slice_values, mode_perms, owner_map):
    groups = lax.axis_size("stem")
    cuts = lax.axis_size("cuts")
    rows, width, half = stems.shape[2], stems.shape[4], closing.shape[3]
    high, narrow, piece = rows // groups, width // groups, half // cuts
    chosen = slice_values[0]
    begun = absorb(stems[0, 0], mode_perms[0], branches[0, chosen[0]])
    begun = begun.reshape(high, groups, 2, groups, narrow)
    state = jnp.transpose(begun, (3, 0, 2, 1, 4)).reshape(rows, 2, width)
    mixed = absorb(state, mode_perms[1], branches[1, chosen[1]])
    leaving = jnp.transpose(mixed.reshape(groups, high, 2, groups, narrow), (3, 0, 1, 2, 4))
    arrived = lax.all_to_all(leaving, "stem", split_axis=0, concat_axis=0, tiled=True)
    arrived = jnp.transpose(arrived, (1, 0, 2, 3, 4)).reshape(groups, high, groups, 2, narrow)
    state = jnp.transpose(arrived, (0, 1, 3, 2, 4)).reshape(rows, 2, width)
    final = absorb(state, mode_perms[2], closing[chosen[2]]).reshape(rows, 2, cuts, piece)
    send = jnp.transpose(jnp.take(final, owner_map, axis=2), (2, 1, 3, 0))
    received = lax.all_to_all(send, "cuts", split_axis=0, concat_axis=0, tiled=True)
    total = jnp.sum(received.reshape(cuts, 2, piece, rows).astype(F32), axis=0)
    return total.reshape(1, 1, 2, piece, rows)


def body(*args):
    groups = lax.axis_size("stem")
    rows, width, half = args[0].shape[2], args[0].shape[4], args[2].shape[3]
    high, narrow = rows // groups, width // groups
    local = high % groups == 0 and high % 16 == 0 and LANES % narrow == 0 and groups % (LANES // narrow) == 0
    local = local and 2 * half == LANES * lax.axis_size("cuts") and half % LANES == 0 and lax.axis_size("cuts") % 2 == 0
    return local_body(*args) if local else exchange_body(*args)


def solution(mesh):
    in_specs = (P("cuts", "stem", None, None, None), P(), P(), P("cuts", None), P(), P())
    out_specs = P("stem", "cuts", None, None, None)
    return jax.shard_map(body, mesh=mesh, in_specs=in_specs, out_specs=out_specs, check_vma=False)
```

```python
import functools

import jax
import jax.numpy as jnp
from jax import lax
from jax.experimental import pallas as pl
from jax.experimental.pallas import tpu as pltpu
from jax.sharding import PartitionSpec as P

BF16 = jnp.bfloat16
F32 = jnp.float32
LANES = 128


def spread(column, modes):
    result = jnp.zeros_like(column)
    for bit, mode in enumerate(modes):
        moved = jnp.bitwise_and(jnp.right_shift(column, bit), 1)
        result = result + jnp.left_shift(moved, mode)
    return result


def stem_kernel(
    groups, swapped, values_in, perms_in, owners_in, stems, branches, closing, give, keep,
    values, perms, owners, begun, loose, first, second, last, orders, begin, flat, amps, later, pieces, half_way, sems,
):
    rows, width = begin.shape[0] // 2, begin.shape[1]
    half = last.shape[2]
    narrow = width // groups
    high = rows // groups
    count = high // groups
    tiles = width // LANES
    per_tile = LANES // narrow
    chunk = 2 * LANES
    streams = width // chunk
    own = groups // streams
    part_rows = rows // streams

    def start(source, target, place):
        copy = pltpu.make_async_copy(source, target, sems.at[place])
        copy.start()
        return copy

    scalars = [
        start(values_in, values, 0),
        start(perms_in, perms, 1),
        start(owners_in, owners, 2),
    ]
    arriving = start(stems, begun, 5)
    pairs = [start(branches.at[0, :, q], first.at[:, q], 6 + q) for q in range(2)]
    for copy in scalars:
        copy.wait()
    middle = start(branches.at[1, values[0, 1]], second, 3)
    final = start(closing.at[values[0, 2]], last, 4)

    column = lax.broadcasted_iota(jnp.int32, (1, width), 1)
    packed = 16
    entry = lax.broadcasted_iota(jnp.int32, (packed, width), 0)

    def make_order(step):
        source = spread(column, [perms[step, bit] for bit in range(perms.shape[1])])
        wanted = (jnp.broadcast_to(source, (packed, width)) - entry).astype(jnp.int16)
        for block in range(width // packed):
            orders[step, block * packed : (block + 1) * packed] = jnp.where(
                wanted == jnp.int16(block * packed), jnp.ones((), BF16), jnp.zeros((), BF16)
            )

    def permute(step, state):
        permuted = jnp.dot(state, orders[step], preferred_element_type=F32).astype(BF16)
        part = permuted.shape[0] // 2
        re, im = permuted[:part], permuted[part:]
        return permuted, jnp.concatenate([-im, re], axis=0)

    def product(factors, pair):
        state = jnp.concatenate(factors, axis=1)
        return jnp.dot(state, pair[...].reshape(-1, pair.shape[2]), preferred_element_type=F32)

    def relabel(taken, target, at, row):
        lane = lax.broadcasted_iota(jnp.int32, taken[0].shape, 1) // narrow
        blocks = []
        for g in range(per_tile):
            block = taken[g]
            for k in range(per_tile):
                if k != g:
                    moved = pltpu.roll(taken[k], ((k - g) % per_tile) * narrow, 1)
                    block = jnp.where(lane == k, moved, block)
            blocks.append(block)
        block = jnp.concatenate(blocks, axis=0).astype(BF16)
        target[row : row + block.shape[0], at * LANES : (at + 1) * LANES] = block

    def relabel_first(stream, y):
        for k in range(chunk // LANES):
            for part in range(2):
                for at in range(tiles):
                    taken = [
                        y[part * rows + l * high : part * rows + (l + 1) * high, k * LANES : (k + 1) * LANES]
                        for l in range(at * per_tile, (at + 1) * per_tile)
                    ]
                    relabel(taken, flat.at[stream], at, part * part_rows + k * per_tile * high)

    def relabel_second(stream, y):
        for tile in range(tiles):
            amps[stream, tile] = y[:, tile * LANES : (tile + 1) * LANES]
        for tile in range(tiles):
            for part in range(2):
                for at in range(tiles):
                    taken = [
                        amps[stream, tile, pl.ds(part * part_rows + l, own * count, stride=groups), :]
                        for l in range(at * per_tile, (at + 1) * per_tile)
                    ]
                    relabel(taken, later.at[stream], at, part * part_rows + tile * per_tile * own * count)

    make_order(0)
    arriving.wait()
    deep = 2 * tiles * high
    for l in range(groups):
        loose[l * deep : (l + 1) * deep] = begun[:, l].astype(F32).reshape(deep, LANES)
    for part in range(2):
        for tile in range(tiles):
            taken = loose[pl.ds(2 * tile + part, rows, stride=2 * tiles), :]
            begin[part * rows : (part + 1) * rows, tile * LANES : (tile + 1) * LANES] = taken.astype(BF16)
    factors = permute(0, begin[...])
    make_order(1)
    make_order(2)
    chosen = first.at[values[0, 0]]
    pairs[0].wait()
    for i in range(streams):
        half_way[i] = jnp.dot(factors[0], chosen[0, :, i * chunk : (i + 1) * chunk], preferred_element_type=F32)
    pairs[1].wait()
    y = [
        half_way[i] + jnp.dot(factors[1], chosen[1, :, i * chunk : (i + 1) * chunk], preferred_element_type=F32)
        for i in range(streams)
    ]
    state = []
    for i in range(streams):
        relabel_first(i, y[i])
        state.append(permute(1, flat[i]))
    middle.wait()
    final.wait()
    y = [product(state[i], second) for i in range(streams)]
    state = []
    for i in range(streams):
        relabel_second(i, y[i])
        state.append(permute(2, later[i]))
    piece = LANES // 2
    wide = lax.broadcasted_iota(jnp.int32, (part_rows, LANES), 1) < piece
    depth = own * count
    for i in range(streams):
        y = product(state[i], last)
        for tile in range(half // LANES):
            re = y[:part_rows, tile * LANES : (tile + 1) * LANES]
            im = y[part_rows:, tile * LANES : (tile + 1) * LANES]
            for k, block in enumerate(
                (jnp.where(wide, re, pltpu.roll(im, piece, 1)), jnp.where(wide, pltpu.roll(re, piece, 1), im))
            ):
                pieces[2 * tile + k, :, i * depth : (i + 1) * depth] = block.reshape(groups, depth, LANES).astype(BF16)
    mine, group_rows = lax.axis_index("cuts"), rows // groups
    team = mine % 2
    for pair, group in swapped:
        team = jnp.where((mine // 2 == pair) & (lax.axis_index("stem") == group), 1 - team, team)
    for pair in range(give.shape[0]):
        give[pair] = pieces[owners[2 * pair + 1 - team]].reshape(rows, LANES)
        keep[pair] = pieces[owners[2 * pair + team]].reshape(rows, LANES)
    for pair, group in swapped:
        place = slice(group * group_rows, (group + 1) * group_rows)
        give[pair, place] = pieces[owners[2 * pair + team], group]
        keep[pair, place] = pieces[owners[2 * pair + 1 - team], group]


def pair_kernel(order, high, keep, came, send):
    for place, (pair, group) in enumerate(order):
        rows = slice(group * high, (group + 1) * high)
        total = keep[pair, rows].astype(F32) + came[pair, rows].astype(F32)
        send[place] = total.astype(BF16)


def sum_kernel(order, groups, received, total):
    high, columns = received.shape[1], total.shape[1]
    count = high // groups
    row = lax.broadcasted_iota(jnp.int32, (high, columns), 0)
    first = (row // count) * (groups * count) + row % count
    distance = (lax.broadcasted_iota(jnp.int32, (high, columns), 1) - first).astype(jnp.int16)
    chosen = [
        jnp.where(distance == jnp.int16(group * count), jnp.ones((), BF16), jnp.zeros((), BF16)) for _, group in order
    ]
    total[...] = lax.dot_general(
        received[...].reshape(-1, LANES),
        jnp.concatenate(chosen, axis=0),
        (((0,), (0,)), ((), ())),
        preferred_element_type=F32,
    )


def group_order(pairs, groups):
    order = [(pair, group) for pair in range(pairs) for group in range(groups)]
    order.insert(0, order.pop(-min(3, len(order))))
    return order


def local_body(stems, branches, closing, slice_values, mode_perms, owner_map):
    groups = lax.axis_size("stem")
    cuts = lax.axis_size("cuts")
    rows, width, half = stems.shape[2], stems.shape[4], closing.shape[3]
    high = rows // groups
    state = jnp.transpose(stems.reshape(rows, 2, width // LANES, LANES), (0, 2, 1, 3)).reshape(high, groups, -1, LANES)
    vmem, hbm = pl.BlockSpec(memory_space=pltpu.VMEM), pl.BlockSpec(memory_space=pl.ANY)
    streams = width // (2 * LANES)
    swapped = [(0, 0)]
    half_shape = pltpu.VMEM((cuts // 2, rows, LANES), BF16)
    give, keep = pl.pallas_call(
        functools.partial(stem_kernel, groups, swapped),
        out_shape=(half_shape, half_shape),
        in_specs=[hbm] * 6,
        out_specs=(vmem, vmem),
        scratch_shapes=[
            pltpu.SMEM(slice_values.shape, jnp.int32),
            pltpu.SMEM(mode_perms.shape, jnp.int32),
            pltpu.SMEM(owner_map.shape, jnp.int32),
            pltpu.VMEM(state.shape, BF16),
            pltpu.VMEM((2 * rows * width // LANES, LANES), F32),
            pltpu.VMEM(branches.shape[1:], BF16),
            pltpu.VMEM(branches.shape[2:], BF16),
            pltpu.VMEM(closing.shape[1:], BF16),
            pltpu.VMEM((3, width, width), BF16),
            pltpu.VMEM((2 * rows, width), BF16),
            pltpu.VMEM((streams, 2 * rows // streams, width), BF16),
            pltpu.VMEM((streams, width // LANES, 2 * rows // streams, LANES), F32),
            pltpu.VMEM((streams, 2 * rows // streams, width), BF16),
            pltpu.VMEM((cuts, groups, high, LANES), BF16),
            pltpu.VMEM((streams, 2 * rows, width // streams), F32),
            pltpu.SemaphoreType.DMA((8,)),
        ],
        name="stem",
    )(slice_values, mode_perms, owner_map, state, branches, closing)
    came = lax.ppermute(give, "cuts", [(i, i ^ 1) for i in range(cuts)])
    order = group_order(cuts // 2, groups)
    in_vmem = lambda x: pltpu.with_memory_space_constraint(x, pltpu.VMEM)
    send = pl.pallas_call(
        functools.partial(pair_kernel, order, high),
        out_shape=pltpu.VMEM((len(order), high, LANES), BF16),
        in_specs=[vmem, vmem],
        out_specs=vmem,
        name="pair",
    )(in_vmem(keep), in_vmem(came))
    members = [
        [(2 * pair + (team ^ ((pair, group) in swapped))) * groups + group for pair, group in order]
        for team in range(2)
    ]
    received = lax.all_to_all(
        send, ("cuts", "stem"), split_axis=0, concat_axis=0, axis_index_groups=members, tiled=True
    )
    total = pl.pallas_call(
        functools.partial(sum_kernel, order, groups),
        out_shape=jax.ShapeDtypeStruct((LANES, rows), F32),
        in_specs=[vmem],
        out_specs=vmem,
        name="total",
    )(in_vmem(received))
    return total.reshape(1, 1, 2, half // cuts, rows)


def absorb(state, perm, pair):
    width = pair.shape[1]
    column = jnp.arange(width, dtype=jnp.int32)
    source = spread(column, [perm[bit] for bit in range(perm.shape[0])])
    order = (column[:, None] == source[None, :]).astype(BF16)
    permuted = jnp.einsum("rpi,ij->prj", state, order, preferred_element_type=F32).astype(BF16)
    product = jnp.einsum("prj,qjk->pqrk", permuted, pair, preferred_element_type=F32)
    return jnp.stack([product[0, 0] - product[1, 1], product[0, 1] + product[1, 0]], axis=1).astype(BF16)


def exchange_body(stems, branches, closing, slice_values, mode_perms, owner_map):
    groups = lax.axis_size("stem")
    cuts = lax.axis_size("cuts")
    rows, width, half = stems.shape[2], stems.shape[4], closing.shape[3]
    high, narrow, piece = rows // groups, width // groups, half // cuts
    chosen = slice_values[0]
    begun = absorb(stems[0, 0], mode_perms[0], branches[0, chosen[0]])
    begun = begun.reshape(high, groups, 2, groups, narrow)
    state = jnp.transpose(begun, (3, 0, 2, 1, 4)).reshape(rows, 2, width)
    mixed = absorb(state, mode_perms[1], branches[1, chosen[1]])
    leaving = jnp.transpose(mixed.reshape(groups, high, 2, groups, narrow), (3, 0, 1, 2, 4))
    arrived = lax.all_to_all(leaving, "stem", split_axis=0, concat_axis=0, tiled=True)
    arrived = jnp.transpose(arrived, (1, 0, 2, 3, 4)).reshape(groups, high, groups, 2, narrow)
    state = jnp.transpose(arrived, (0, 1, 3, 2, 4)).reshape(rows, 2, width)
    final = absorb(state, mode_perms[2], closing[chosen[2]]).reshape(rows, 2, cuts, piece)
    send = jnp.transpose(jnp.take(final, owner_map, axis=2), (2, 1, 3, 0))
    received = lax.all_to_all(send, "cuts", split_axis=0, concat_axis=0, tiled=True)
    total = jnp.sum(received.reshape(cuts, 2, piece, rows).astype(F32), axis=0)
    return total.reshape(1, 1, 2, piece, rows)


def body(*args):
    groups = lax.axis_size("stem")
    rows, width, half = args[0].shape[2], args[0].shape[4], args[2].shape[3]
    high, narrow = rows // groups, width // groups
    local = high % groups == 0 and high % 16 == 0 and LANES % narrow == 0 and groups % (LANES // narrow) == 0
    local = local and 2 * half == LANES * lax.axis_size("cuts") and half % LANES == 0 and lax.axis_size("cuts") % 2 == 0
    return local_body(*args) if local else exchange_body(*args)


def solution(mesh):
    in_specs = (P("cuts", "stem", None, None, None), P(), P(), P("cuts", None), P(), P())
    out_specs = P("stem", "cuts", None, None, None)
    return jax.shard_map(body, mesh=mesh, in_specs=in_specs, out_specs=out_specs, check_vma=False)
```

```python
import functools

import jax
import jax.numpy as jnp
from jax import lax
from jax.experimental import pallas as pl
from jax.experimental.pallas import tpu as pltpu
from jax.sharding import PartitionSpec as P

BF16 = jnp.bfloat16
F32 = jnp.float32
LANES = 128


def spread(column, modes):
    result = jnp.zeros_like(column)
    for bit, mode in enumerate(modes):
        moved = jnp.bitwise_and(jnp.right_shift(column, bit), 1)
        result = result + jnp.left_shift(moved, mode)
    return result


def stem_kernel(
    groups, swapped, values_in, perms_in, owners_in, stems, branches, closing, give, keep,
    values, perms, owners, begun, loose, first, second, last, orders, begin, flat, amps, later, pieces, half_way, sems,
):
    rows, width = begin.shape[0] // 2, begin.shape[1]
    half = last.shape[2]
    narrow = width // groups
    high = rows // groups
    count = high // groups
    tiles = width // LANES
    per_tile = LANES // narrow
    chunk = 2 * LANES
    streams = width // chunk
    own = groups // streams
    part_rows = rows // streams

    def start(source, target, place):
        copy = pltpu.make_async_copy(source, target, sems.at[place])
        copy.start()
        return copy

    scalars = [
        start(values_in, values, 0),
        start(perms_in, perms, 1),
        start(owners_in, owners, 2),
    ]
    arriving = start(stems, begun, 5)
    pairs = [start(branches.at[0, :, q], first.at[:, q], 6 + q) for q in range(2)]
    for copy in scalars:
        copy.wait()
    middle = start(branches.at[1, values[0, 1]], second, 3)
    final = start(closing.at[values[0, 2]], last, 4)

    column = lax.broadcasted_iota(jnp.int32, (1, width), 1)
    packed = 16
    entry = lax.broadcasted_iota(jnp.int32, (packed, width), 0)

    def make_order(step):
        source = spread(column, [perms[step, bit] for bit in range(perms.shape[1])])
        wanted = (jnp.broadcast_to(source, (packed, width)) - entry).astype(jnp.int16)
        for block in range(width // packed):
            orders[step, block * packed : (block + 1) * packed] = jnp.where(
                wanted == jnp.int16(block * packed), jnp.ones((), BF16), jnp.zeros((), BF16)
            )

    def permute(step, state):
        permuted = jnp.dot(state, orders[step], preferred_element_type=F32).astype(BF16)
        part = permuted.shape[0] // 2
        re, im = permuted[:part], permuted[part:]
        return permuted, jnp.concatenate([-im, re], axis=0)

    def product(factors, pair):
        state = jnp.concatenate(factors, axis=1)
        return jnp.dot(state, pair[...].reshape(-1, pair.shape[2]), preferred_element_type=F32)

    def relabel(taken, target, at, row):
        lane = lax.broadcasted_iota(jnp.int32, taken[0].shape, 1) // narrow
        blocks = []
        for g in range(per_tile):
            block = taken[g]
            for k in range(per_tile):
                if k != g:
                    moved = pltpu.roll(taken[k], ((k - g) % per_tile) * narrow, 1)
                    block = jnp.where(lane == k, moved, block)
            blocks.append(block)
        block = jnp.concatenate(blocks, axis=0).astype(BF16)
        target[row : row + block.shape[0], at * LANES : (at + 1) * LANES] = block

    def relabel_first(stream, y):
        for k in range(chunk // LANES):
            for part in range(2):
                for at in range(tiles):
                    taken = [
                        y[part * rows + l * high : part * rows + (l + 1) * high, k * LANES : (k + 1) * LANES]
                        for l in range(at * per_tile, (at + 1) * per_tile)
                    ]
                    relabel(taken, flat.at[stream], at, part * part_rows + k * per_tile * high)

    def relabel_second(stream, y):
        for tile in range(tiles):
            amps[stream, tile] = y[:, tile * LANES : (tile + 1) * LANES]
        for tile in range(tiles):
            for part in range(2):
                for at in range(tiles):
                    taken = [
                        amps[stream, tile, pl.ds(part * part_rows + l, own * count, stride=groups), :]
                        for l in range(at * per_tile, (at + 1) * per_tile)
                    ]
                    relabel(taken, later.at[stream], at, part * part_rows + tile * per_tile * own * count)

    make_order(0)
    arriving.wait()
    deep = 2 * tiles * high
    for l in range(groups):
        loose[l * deep : (l + 1) * deep] = begun[:, l].astype(F32).reshape(deep, LANES)
    for part in range(2):
        for tile in range(tiles):
            taken = loose[pl.ds(2 * tile + part, rows, stride=2 * tiles), :]
            begin[part * rows : (part + 1) * rows, tile * LANES : (tile + 1) * LANES] = taken.astype(BF16)
    factors = permute(0, begin[...])
    make_order(1)
    make_order(2)
    chosen = first.at[values[0, 0]]
    pairs[0].wait()
    for i in range(streams):
        half_way[i] = jnp.dot(factors[0], chosen[0, :, i * chunk : (i + 1) * chunk], preferred_element_type=F32)
    pairs[1].wait()
    y = [
        half_way[i] + jnp.dot(factors[1], chosen[1, :, i * chunk : (i + 1) * chunk], preferred_element_type=F32)
        for i in range(streams)
    ]
    state = []
    for i in range(streams):
        relabel_first(i, y[i])
        state.append(permute(1, flat[i]))
    middle.wait()
    final.wait()
    y = [product(state[i], second) for i in range(streams)]
    state = []
    for i in range(streams):
        relabel_second(i, y[i])
        state.append(permute(2, later[i]))
    piece = LANES // 2
    wide = lax.broadcasted_iota(jnp.int32, (part_rows, LANES), 1) < piece
    depth = own * count
    for i in range(streams):
        y = product(state[i], last)
        for tile in range(half // LANES):
            re = y[:part_rows, tile * LANES : (tile + 1) * LANES]
            im = y[part_rows:, tile * LANES : (tile + 1) * LANES]
            for k, block in enumerate(
                (jnp.where(wide, re, pltpu.roll(im, piece, 1)), jnp.where(wide, pltpu.roll(re, piece, 1), im))
            ):
                pieces[2 * tile + k, :, i * depth : (i + 1) * depth] = block.reshape(groups, depth, LANES).astype(BF16)
    mine, group_rows = lax.axis_index("cuts"), rows // groups
    team = mine % 2
    for pair, group in swapped:
        team = jnp.where((mine // 2 == pair) & (lax.axis_index("stem") == group), 1 - team, team)
    for pair in range(give.shape[0]):
        give[pair] = pieces[owners[2 * pair + 1 - team]].reshape(rows, LANES)
        keep[pair] = pieces[owners[2 * pair + team]].reshape(rows, LANES)
    for pair, group in swapped:
        place = slice(group * group_rows, (group + 1) * group_rows)
        give[pair, place] = pieces[owners[2 * pair + team], group]
        keep[pair, place] = pieces[owners[2 * pair + 1 - team], group]


def pair_kernel(order, high, keep, came, send):
    for place, (pair, group) in enumerate(order):
        rows = slice(group * high, (group + 1) * high)
        total = keep[pair, rows].astype(F32) + came[pair, rows].astype(F32)
        send[place] = total.astype(BF16)


def sum_kernel(order, groups, received, total, held):
    high = received.shape[1]
    count = high // groups
    for group in range(groups):
        block = sum(received[at].astype(F32) for at, (_, g) in enumerate(order) if g == group)
        for t in range(groups):
            row = t * groups * count + group * count
            held[row : row + count] = block[t * count : (t + 1) * count]
    total[...] = held[...].T


def group_order(pairs, groups):
    order = [(pair, group) for pair in range(pairs) for group in range(groups)]
    order.insert(0, order.pop(-min(3, len(order))))
    return order


def local_body(stems, branches, closing, slice_values, mode_perms, owner_map):
    groups = lax.axis_size("stem")
    cuts = lax.axis_size("cuts")
    rows, width, half = stems.shape[2], stems.shape[4], closing.shape[3]
    high = rows // groups
    state = jnp.transpose(stems.reshape(rows, 2, width // LANES, LANES), (0, 2, 1, 3)).reshape(high, groups, -1, LANES)
    vmem, hbm = pl.BlockSpec(memory_space=pltpu.VMEM), pl.BlockSpec(memory_space=pl.ANY)
    streams = width // (2 * LANES)
    swapped = [(0, 0)]
    half_shape = pltpu.VMEM((cuts // 2, rows, LANES), BF16)
    give, keep = pl.pallas_call(
        functools.partial(stem_kernel, groups, swapped),
        out_shape=(half_shape, half_shape),
        in_specs=[hbm] * 6,
        out_specs=(vmem, vmem),
        scratch_shapes=[
            pltpu.SMEM(slice_values.shape, jnp.int32),
            pltpu.SMEM(mode_perms.shape, jnp.int32),
            pltpu.SMEM(owner_map.shape, jnp.int32),
            pltpu.VMEM(state.shape, BF16),
            pltpu.VMEM((2 * rows * width // LANES, LANES), F32),
            pltpu.VMEM(branches.shape[1:], BF16),
            pltpu.VMEM(branches.shape[2:], BF16),
            pltpu.VMEM(closing.shape[1:], BF16),
            pltpu.VMEM((3, width, width), BF16),
            pltpu.VMEM((2 * rows, width), BF16),
            pltpu.VMEM((streams, 2 * rows // streams, width), BF16),
            pltpu.VMEM((streams, width // LANES, 2 * rows // streams, LANES), F32),
            pltpu.VMEM((streams, 2 * rows // streams, width), BF16),
            pltpu.VMEM((cuts, groups, high, LANES), BF16),
            pltpu.VMEM((streams, 2 * rows, width // streams), F32),
            pltpu.SemaphoreType.DMA((8,)),
        ],
        name="stem",
    )(slice_values, mode_perms, owner_map, state, branches, closing)
    came = lax.ppermute(give, "cuts", [(i, i ^ 1) for i in range(cuts)])
    order = group_order(cuts // 2, groups)
    in_vmem = lambda x: pltpu.with_memory_space_constraint(x, pltpu.VMEM)
    send = pl.pallas_call(
        functools.partial(pair_kernel, order, high),
        out_shape=pltpu.VMEM((len(order), high, LANES), BF16),
        in_specs=[vmem, vmem],
        out_specs=vmem,
        name="pair",
    )(in_vmem(keep), in_vmem(came))
    members = [
        [(2 * pair + (team ^ ((pair, group) in swapped))) * groups + group for pair, group in order]
        for team in range(2)
    ]
    received = lax.all_to_all(
        send, ("cuts", "stem"), split_axis=0, concat_axis=0, axis_index_groups=members, tiled=True
    )
    total = pl.pallas_call(
        functools.partial(sum_kernel, order, groups),
        out_shape=jax.ShapeDtypeStruct((LANES, rows), F32),
        in_specs=[vmem],
        out_specs=vmem,
        scratch_shapes=[pltpu.VMEM((rows, LANES), F32)],
        name="total",
    )(in_vmem(received))
    return total.reshape(1, 1, 2, half // cuts, rows)


def absorb(state, perm, pair):
    width = pair.shape[1]
    column = jnp.arange(width, dtype=jnp.int32)
    source = spread(column, [perm[bit] for bit in range(perm.shape[0])])
    order = (column[:, None] == source[None, :]).astype(BF16)
    permuted = jnp.einsum("rpi,ij->prj", state, order, preferred_element_type=F32).astype(BF16)
    product = jnp.einsum("prj,qjk->pqrk", permuted, pair, preferred_element_type=F32)
    return jnp.stack([product[0, 0] - product[1, 1], product[0, 1] + product[1, 0]], axis=1).astype(BF16)


def exchange_body(stems, branches, closing, slice_values, mode_perms, owner_map):
    groups = lax.axis_size("stem")
    cuts = lax.axis_size("cuts")
    rows, width, half = stems.shape[2], stems.shape[4], closing.shape[3]
    high, narrow, piece = rows // groups, width // groups, half // cuts
    chosen = slice_values[0]
    begun = absorb(stems[0, 0], mode_perms[0], branches[0, chosen[0]])
    begun = begun.reshape(high, groups, 2, groups, narrow)
    state = jnp.transpose(begun, (3, 0, 2, 1, 4)).reshape(rows, 2, width)
    mixed = absorb(state, mode_perms[1], branches[1, chosen[1]])
    leaving = jnp.transpose(mixed.reshape(groups, high, 2, groups, narrow), (3, 0, 1, 2, 4))
    arrived = lax.all_to_all(leaving, "stem", split_axis=0, concat_axis=0, tiled=True)
    arrived = jnp.transpose(arrived, (1, 0, 2, 3, 4)).reshape(groups, high, groups, 2, narrow)
    state = jnp.transpose(arrived, (0, 1, 3, 2, 4)).reshape(rows, 2, width)
    final = absorb(state, mode_perms[2], closing[chosen[2]]).reshape(rows, 2, cuts, piece)
    send = jnp.transpose(jnp.take(final, owner_map, axis=2), (2, 1, 3, 0))
    received = lax.all_to_all(send, "cuts", split_axis=0, concat_axis=0, tiled=True)
    total = jnp.sum(received.reshape(cuts, 2, piece, rows).astype(F32), axis=0)
    return total.reshape(1, 1, 2, piece, rows)


def body(*args):
    groups = lax.axis_size("stem")
    rows, width, half = args[0].shape[2], args[0].shape[4], args[2].shape[3]
    high, narrow = rows // groups, width // groups
    local = high % groups == 0 and high % 16 == 0 and LANES % narrow == 0 and groups % (LANES // narrow) == 0
    local = local and 2 * half == LANES * lax.axis_size("cuts") and half % LANES == 0 and lax.axis_size("cuts") % 2 == 0
    return local_body(*args) if local else exchange_body(*args)


def solution(mesh):
    in_specs = (P("cuts", "stem", None, None, None), P(), P(), P("cuts", None), P(), P())
    out_specs = P("stem", "cuts", None, None, None)
    return jax.shard_map(body, mesh=mesh, in_specs=in_specs, out_specs=out_specs, check_vma=False)
```

```python
import functools

import jax
import jax.numpy as jnp
from jax import lax
from jax.experimental import pallas as pl
from jax.experimental.pallas import tpu as pltpu
from jax.sharding import PartitionSpec as P

BF16 = jnp.bfloat16
F32 = jnp.float32
LANES = 128


def spread(column, modes):
    result = jnp.zeros_like(column)
    for bit, mode in enumerate(modes):
        moved = jnp.bitwise_and(jnp.right_shift(column, bit), 1)
        result = result + jnp.left_shift(moved, mode)
    return result


def stem_kernel(
    groups, swapped, values_in, perms_in, owners_in, stems, branches, closing, give, keep,
    values, perms, owners, begun, loose, first, second, last, orders, begin, flat, amps, later, pieces, half_way, sems,
):
    rows, width = begin.shape[0] // 2, begin.shape[1]
    half = last.shape[2]
    narrow = width // groups
    high = rows // groups
    count = high // groups
    tiles = width // LANES
    per_tile = LANES // narrow
    chunk = 2 * LANES
    streams = width // chunk
    own = groups // streams
    part_rows = rows // streams

    def start(source, target, place, priority=0):
        copy = pltpu.make_async_copy(source, target, sems.at[place])
        copy.start(priority=priority)
        return copy

    scalars = [
        start(values_in, values, 0),
        start(perms_in, perms, 1),
        start(owners_in, owners, 2),
    ]
    arriving = start(stems, begun, 5, 0)
    pairs = [start(branches.at[0, :, q], first.at[:, q], 6 + q, (0, 0)[q]) for q in range(2)]
    for copy in scalars:
        copy.wait()
    middle = start(branches.at[1, values[0, 1]], second, 3, 1)
    final = start(closing.at[values[0, 2]], last, 4, 1)

    column = lax.broadcasted_iota(jnp.int32, (1, width), 1)
    packed = 16
    entry = lax.broadcasted_iota(jnp.int32, (packed, width), 0)

    def make_order(step):
        source = spread(column, [perms[step, bit] for bit in range(perms.shape[1])])
        wanted = (jnp.broadcast_to(source, (packed, width)) - entry).astype(jnp.int16)
        for block in range(width // packed):
            orders[step, block * packed : (block + 1) * packed] = jnp.where(
                wanted == jnp.int16(block * packed), jnp.ones((), BF16), jnp.zeros((), BF16)
            )

    def permute(step, state):
        permuted = jnp.dot(state, orders[step], preferred_element_type=F32).astype(BF16)
        part = permuted.shape[0] // 2
        re, im = permuted[:part], permuted[part:]
        return permuted, jnp.concatenate([-im, re], axis=0)

    def product(factors, pair):
        state = jnp.concatenate(factors, axis=1)
        return jnp.dot(state, pair[...].reshape(-1, pair.shape[2]), preferred_element_type=F32)

    def relabel(taken, target, at, row):
        lane = lax.broadcasted_iota(jnp.int32, taken[0].shape, 1) // narrow
        blocks = []
        for g in range(per_tile):
            block = taken[g]
            for k in range(per_tile):
                if k != g:
                    moved = pltpu.roll(taken[k], ((k - g) % per_tile) * narrow, 1)
                    block = jnp.where(lane == k, moved, block)
            blocks.append(block)
        block = jnp.concatenate(blocks, axis=0).astype(BF16)
        target[row : row + block.shape[0], at * LANES : (at + 1) * LANES] = block

    def relabel_first(stream, y):
        for k in range(chunk // LANES):
            for part in range(2):
                for at in range(tiles):
                    taken = [
                        y[part * rows + l * high : part * rows + (l + 1) * high, k * LANES : (k + 1) * LANES]
                        for l in range(at * per_tile, (at + 1) * per_tile)
                    ]
                    relabel(taken, flat.at[stream], at, part * part_rows + k * per_tile * high)

    def relabel_second(stream, y):
        for tile in range(tiles):
            amps[stream, tile] = y[:, tile * LANES : (tile + 1) * LANES]
        for tile in range(tiles):
            for part in range(2):
                for at in range(tiles):
                    taken = [
                        amps[stream, tile, pl.ds(part * part_rows + l, own * count, stride=groups), :]
                        for l in range(at * per_tile, (at + 1) * per_tile)
                    ]
                    relabel(taken, later.at[stream], at, part * part_rows + tile * per_tile * own * count)

    make_order(0)
    arriving.wait()
    deep = 2 * tiles * high
    for l in range(groups):
        loose[l * deep : (l + 1) * deep] = begun[:, l].astype(F32).reshape(deep, LANES)
    for part in range(2):
        for tile in range(tiles):
            taken = loose[pl.ds(2 * tile + part, rows, stride=2 * tiles), :]
            begin[part * rows : (part + 1) * rows, tile * LANES : (tile + 1) * LANES] = taken.astype(BF16)
    factors = permute(0, begin[...])
    make_order(1)
    make_order(2)
    chosen = first.at[values[0, 0]]
    pairs[0].wait()
    for i in range(streams):
        half_way[i] = jnp.dot(factors[0], chosen[0, :, i * chunk : (i + 1) * chunk], preferred_element_type=F32)
    pairs[1].wait()
    y = [
        half_way[i] + jnp.dot(factors[1], chosen[1, :, i * chunk : (i + 1) * chunk], preferred_element_type=F32)
        for i in range(streams)
    ]
    state = []
    for i in range(streams):
        relabel_first(i, y[i])
        state.append(permute(1, flat[i]))
    middle.wait()
    final.wait()
    y = [product(state[i], second) for i in range(streams)]
    state = []
    for i in range(streams):
        relabel_second(i, y[i])
        state.append(permute(2, later[i]))
    piece = LANES // 2
    wide = lax.broadcasted_iota(jnp.int32, (part_rows, LANES), 1) < piece
    depth = own * count
    for i in range(streams):
        y = product(state[i], last)
        for tile in range(half // LANES):
            re = y[:part_rows, tile * LANES : (tile + 1) * LANES]
            im = y[part_rows:, tile * LANES : (tile + 1) * LANES]
            for k, block in enumerate(
                (jnp.where(wide, re, pltpu.roll(im, piece, 1)), jnp.where(wide, pltpu.roll(re, piece, 1), im))
            ):
                pieces[2 * tile + k, :, i * depth : (i + 1) * depth] = block.reshape(groups, depth, LANES).astype(BF16)
    mine, group_rows = lax.axis_index("cuts"), rows // groups
    team = mine % 2
    for pair, group in swapped:
        team = jnp.where((mine // 2 == pair) & (lax.axis_index("stem") == group), 1 - team, team)
    for pair in range(give.shape[0]):
        give[pair] = pieces[owners[2 * pair + 1 - team]].reshape(rows, LANES)
        keep[pair] = pieces[owners[2 * pair + team]].reshape(rows, LANES)
    for pair, group in swapped:
        place = slice(group * group_rows, (group + 1) * group_rows)
        give[pair, place] = pieces[owners[2 * pair + team], group]
        keep[pair, place] = pieces[owners[2 * pair + 1 - team], group]


def pair_kernel(order, high, keep, came, send):
    for place, (pair, group) in enumerate(order):
        rows = slice(group * high, (group + 1) * high)
        total = keep[pair, rows].astype(F32) + came[pair, rows].astype(F32)
        send[place] = total.astype(BF16)


def sum_kernel(order, groups, received, total, held):
    high = received.shape[1]
    count = high // groups
    for group in range(groups):
        block = sum(received[at].astype(F32) for at, (_, g) in enumerate(order) if g == group)
        for t in range(groups):
            row = t * groups * count + group * count
            held[row : row + count] = block[t * count : (t + 1) * count]
    total[...] = held[...].T


def group_order(pairs, groups):
    order = [(pair, group) for pair in range(pairs) for group in range(groups)]
    order.insert(0, order.pop(-min(3, len(order))))
    return order


def local_body(stems, branches, closing, slice_values, mode_perms, owner_map):
    groups = lax.axis_size("stem")
    cuts = lax.axis_size("cuts")
    rows, width, half = stems.shape[2], stems.shape[4], closing.shape[3]
    high = rows // groups
    state = jnp.transpose(stems.reshape(rows, 2, width // LANES, LANES), (0, 2, 1, 3)).reshape(high, groups, -1, LANES)
    vmem, hbm = pl.BlockSpec(memory_space=pltpu.VMEM), pl.BlockSpec(memory_space=pl.ANY)
    streams = width // (2 * LANES)
    swapped = [(0, 0)]
    half_shape = pltpu.VMEM((cuts // 2, rows, LANES), BF16)
    give, keep = pl.pallas_call(
        functools.partial(stem_kernel, groups, swapped),
        out_shape=(half_shape, half_shape),
        in_specs=[hbm] * 6,
        out_specs=(vmem, vmem),
        scratch_shapes=[
            pltpu.SMEM(slice_values.shape, jnp.int32),
            pltpu.SMEM(mode_perms.shape, jnp.int32),
            pltpu.SMEM(owner_map.shape, jnp.int32),
            pltpu.VMEM(state.shape, BF16),
            pltpu.VMEM((2 * rows * width // LANES, LANES), F32),
            pltpu.VMEM(branches.shape[1:], BF16),
            pltpu.VMEM(branches.shape[2:], BF16),
            pltpu.VMEM(closing.shape[1:], BF16),
            pltpu.VMEM((3, width, width), BF16),
            pltpu.VMEM((2 * rows, width), BF16),
            pltpu.VMEM((streams, 2 * rows // streams, width), BF16),
            pltpu.VMEM((streams, width // LANES, 2 * rows // streams, LANES), F32),
            pltpu.VMEM((streams, 2 * rows // streams, width), BF16),
            pltpu.VMEM((cuts, groups, high, LANES), BF16),
            pltpu.VMEM((streams, 2 * rows, width // streams), F32),
            pltpu.SemaphoreType.DMA((8,)),
        ],
        name="stem",
    )(slice_values, mode_perms, owner_map, state, branches, closing)
    came = lax.ppermute(give, "cuts", [(i, i ^ 1) for i in range(cuts)])
    order = group_order(cuts // 2, groups)
    in_vmem = lambda x: pltpu.with_memory_space_constraint(x, pltpu.VMEM)
    send = pl.pallas_call(
        functools.partial(pair_kernel, order, high),
        out_shape=pltpu.VMEM((len(order), high, LANES), BF16),
        in_specs=[vmem, vmem],
        out_specs=vmem,
        name="pair",
    )(in_vmem(keep), in_vmem(came))
    members = [
        [(2 * pair + (team ^ ((pair, group) in swapped))) * groups + group for pair, group in order]
        for team in range(2)
    ]
    received = lax.all_to_all(
        send, ("cuts", "stem"), split_axis=0, concat_axis=0, axis_index_groups=members, tiled=True
    )
    total = pl.pallas_call(
        functools.partial(sum_kernel, order, groups),
        out_shape=jax.ShapeDtypeStruct((LANES, rows), F32),
        in_specs=[vmem],
        out_specs=vmem,
        scratch_shapes=[pltpu.VMEM((rows, LANES), F32)],
        name="total",
    )(in_vmem(received))
    return total.reshape(1, 1, 2, half // cuts, rows)


def absorb(state, perm, pair):
    width = pair.shape[1]
    column = jnp.arange(width, dtype=jnp.int32)
    source = spread(column, [perm[bit] for bit in range(perm.shape[0])])
    order = (column[:, None] == source[None, :]).astype(BF16)
    permuted = jnp.einsum("rpi,ij->prj", state, order, preferred_element_type=F32).astype(BF16)
    product = jnp.einsum("prj,qjk->pqrk", permuted, pair, preferred_element_type=F32)
    return jnp.stack([product[0, 0] - product[1, 1], product[0, 1] + product[1, 0]], axis=1).astype(BF16)


def exchange_body(stems, branches, closing, slice_values, mode_perms, owner_map):
    groups = lax.axis_size("stem")
    cuts = lax.axis_size("cuts")
    rows, width, half = stems.shape[2], stems.shape[4], closing.shape[3]
    high, narrow, piece = rows // groups, width // groups, half // cuts
    chosen = slice_values[0]
    begun = absorb(stems[0, 0], mode_perms[0], branches[0, chosen[0]])
    begun = begun.reshape(high, groups, 2, groups, narrow)
    state = jnp.transpose(begun, (3, 0, 2, 1, 4)).reshape(rows, 2, width)
    mixed = absorb(state, mode_perms[1], branches[1, chosen[1]])
    leaving = jnp.transpose(mixed.reshape(groups, high, 2, groups, narrow), (3, 0, 1, 2, 4))
    arrived = lax.all_to_all(leaving, "stem", split_axis=0, concat_axis=0, tiled=True)
    arrived = jnp.transpose(arrived, (1, 0, 2, 3, 4)).reshape(groups, high, groups, 2, narrow)
    state = jnp.transpose(arrived, (0, 1, 3, 2, 4)).reshape(rows, 2, width)
    final = absorb(state, mode_perms[2], closing[chosen[2]]).reshape(rows, 2, cuts, piece)
    send = jnp.transpose(jnp.take(final, owner_map, axis=2), (2, 1, 3, 0))
    received = lax.all_to_all(send, "cuts", split_axis=0, concat_axis=0, tiled=True)
    total = jnp.sum(received.reshape(cuts, 2, piece, rows).astype(F32), axis=0)
    return total.reshape(1, 1, 2, piece, rows)


def body(*args):
    groups = lax.axis_size("stem")
    rows, width, half = args[0].shape[2], args[0].shape[4], args[2].shape[3]
    high, narrow = rows // groups, width // groups
    local = high % groups == 0 and high % 16 == 0 and LANES % narrow == 0 and groups % (LANES // narrow) == 0
    local = local and 2 * half == LANES * lax.axis_size("cuts") and half % LANES == 0 and lax.axis_size("cuts") % 2 == 0
    return local_body(*args) if local else exchange_body(*args)


def solution(mesh):
    in_specs = (P("cuts", "stem", None, None, None), P(), P(), P("cuts", None), P(), P())
    out_specs = P("stem", "cuts", None, None, None)
    return jax.shard_map(body, mesh=mesh, in_specs=in_specs, out_specs=out_specs, check_vma=False)
```
